32 devices in a mesh: seq: 8 (over z, core), feat: 4 (over y, x).
Axes of the slice: x: 2, y: 2, z: 4, core: 2. Of those that a mesh axis runs over, the one named last changes fastest.
Arguments:
- activations: bfloat16 [2048, 6144], P('seq', 'feat'), may hold values from -15 to 15
- ridge_scale: float32 [], replicated, may hold values from 0.5 to 2
Outputs:
- whitened: bfloat16 [2048, 6144], P('seq', 'feat')
The draws below stay inside these ranges and needn't reach their ends.
All inputs are finite; a program needn't handle non-finite values.
Results may differ from the reference program's by a relative error of at most 0.0033.
Values sent between devices are 32-bit elements; how exact they have to be, the bound alone decides.
A program may use at most 128 MiB of HBM per device.

```python
import math
import jax
import jax.numpy as jnp
from jax import lax

D = 6144
RANK = 128
TOK_DEV = 256
ITERS = 1
ROOT_STEPS = 12
LEVELS = 3
TOKENS = 2048
N_SEQ = 8


def draw_activations(key, part):
    columns = jnp.exp(jax.random.uniform(jax.random.fold_in(key, 11), (D,), jnp.float32, math.log(0.3), math.log(3.0)))
    noise_rows = jnp.clip(jax.random.normal(jax.random.fold_in(key, 12), (TOKENS, D), jnp.float32), -5.0, 5.0)
    return (noise_rows * columns[None, :]).astype(jnp.bfloat16)


def setup_inputs(seed: int = 0) -> dict:
    streams_of = jax.random.split(jax.random.key(seed), 3)
    activations = draw_activations(jax.random.fold_in(streams_of[2], 71), 0)
    ridge_scale = jnp.clip(jnp.exp(jax.random.uniform(streams_of[1], (), jnp.float32, math.log(0.5), math.log(2.0))), 0.5, 2.0)
    return dict(activations=activations, ridge_scale=ridge_scale)


precise = lax.Precision.HIGHEST

def product(left_matrix, right_matrix):
    return jnp.dot(left_matrix, right_matrix, precision=precise)

def reduce_gram(stacked_gram):
    rank_size = stacked_gram.shape[0] // 2
    identity = jnp.eye(rank_size, dtype=stacked_gram.dtype)
    subspace = jnp.concatenate([identity, identity], axis=0) * 0.7071067811865476
    for repeat in range(ITERS):
        image_cols = product(stacked_gram, subspace)
        factor = jnp.linalg.cholesky(product(image_cols.T, image_cols))
        subspace = jax.scipy.linalg.solve_triangular(factor, image_cols.T, lower=True).T
    quotient = product(subspace.T, product(stacked_gram, subspace))
    quotient = 0.5 * (quotient + quotient.T)
    tail_mass = (jnp.trace(stacked_gram) - jnp.trace(quotient)) / rank_size
    root_factor = jnp.linalg.cholesky(quotient)
    inner_gram = product(root_factor.T, root_factor) + tail_mass * identity
    lower_factor = jnp.linalg.cholesky(inner_gram)
    return jax.scipy.linalg.solve_triangular(lower_factor, product(root_factor.T, subspace.T), lower=True)

def combine(earlier, later):
    own_gram = product(earlier, earlier.T)
    cross_gram = product(earlier, later.T)
    last_gram = product(later, later.T)
    stacked_gram = jnp.concatenate([jnp.concatenate([own_gram, cross_gram], 1), jnp.concatenate([cross_gram.T, last_gram], 1)], 0)
    mixing = reduce_gram(stacked_gram)
    return product(mixing, jnp.concatenate([earlier, later], 0))

def square_root(matrix):
    identity = jnp.eye(matrix.shape[0], dtype=matrix.dtype)
    norm_size = jnp.sqrt(jnp.sum(matrix * matrix))
    current = matrix / norm_size
    partner = identity
    for repeat in range(ROOT_STEPS):
        middle = 1.5 * identity - 0.5 * product(partner, current)
        current = product(current, middle)
        partner = product(middle, partner)
    return current * jnp.sqrt(norm_size)

def whiten(slab_rows, prefix, seen_rows, ridge_scale):
    scaled = prefix * lax.rsqrt(seen_rows * ridge_scale)
    small_gram = product(scaled, scaled.T)
    identity = jnp.eye(small_gram.shape[0], dtype=small_gram.dtype)
    shifted = identity + small_gram
    total_gram = shifted + square_root(shifted)
    total_gram = 0.5 * (total_gram + total_gram.T)
    half_basis = scaled.astype(jnp.bfloat16)
    projection = jnp.dot(slab_rows.astype(jnp.float32), half_basis.T.astype(jnp.float32), preferred_element_type=jnp.float32)
    coefficients = jax.scipy.linalg.cho_solve((jnp.linalg.cholesky(total_gram), True), projection.T).T
    restored = jnp.dot(coefficients.astype(jnp.bfloat16).astype(jnp.float32), half_basis.astype(jnp.float32), preferred_element_type=jnp.float32)
    return ((slab_rows.astype(jnp.float32) - restored) * lax.rsqrt(ridge_scale)).astype(jnp.bfloat16)

def reference(activations, ridge_scale):
    block_count = TOK_DEV // (2 * RANK)
    wide_rows = activations.reshape(N_SEQ * block_count, 2 * RANK, D).astype(jnp.float32)
    slab_grams = jnp.einsum('bik,bjk->bij', wide_rows, wide_rows, precision=precise)
    mixtures = jax.vmap(reduce_gram)(slab_grams)
    sketches = jnp.einsum('bij,bjk->bik', mixtures, wide_rows, precision=precise).reshape(N_SEQ, block_count, RANK, D)
    slab_sketch = sketches[:, 0]
    for block_index in range(1, block_count):
        slab_sketch = jax.vmap(combine)(slab_sketch, sketches[:, block_index])
    seq_index = jnp.arange(N_SEQ, dtype=jnp.int32)
    tree_block = slab_sketch
    prefix = slab_sketch
    for tree_level in range(LEVELS):
        sibling = jnp.bitwise_xor(seq_index, jnp.int32(1 << tree_level))
        partner = tree_block[sibling]
        merged = jax.vmap(combine)(partner, prefix)
        has_bit = seq_index // (1 << tree_level) % 2 == 1
        prefix = jnp.where(has_bit[:, None, None], merged, prefix)
        if tree_level + 1 < LEVELS:
            tree_block = jax.vmap(combine)(tree_block, partner)
    seen_rows = ((seq_index + 1) * TOK_DEV).astype(jnp.float32)
    slabs = activations.reshape(N_SEQ, TOK_DEV, D)
    whitened = jax.vmap(whiten, in_axes=(0, 0, 0, None))(slabs, prefix, seen_rows, ridge_scale)
    return whitened.reshape(N_SEQ * TOK_DEV, D)
```

```python
import functools

import jax
import jax.numpy as jnp
from jax import lax
from jax.experimental import pallas as pl
from jax.experimental.pallas import tpu as pltpu
from jax.sharding import PartitionSpec as P

RANK = 128
ROOT_STEPS = 12
BLOCK = 32
SUB = 16
MESH = pl.DeviceIdType.MESH
HIGHEST = lax.Precision.HIGHEST


def mm(a, b):
    return jnp.dot(a, b, precision=HIGHEST, preferred_element_type=jnp.float32)


def mm_t(a, b):
    return lax.dot_general(
        a, b, (((1,), (1,)), ((), ())), precision=HIGHEST, preferred_element_type=jnp.float32
    )


def split_3(x):
    high = x.astype(jnp.bfloat16)
    rest = x - high.astype(jnp.float32)
    middle = rest.astype(jnp.bfloat16)
    low = (rest - middle.astype(jnp.float32)).astype(jnp.bfloat16)
    return high, middle, low


def eye():
    rows = lax.broadcasted_iota(jnp.int32, (RANK, RANK), 0)
    columns = lax.broadcasted_iota(jnp.int32, (RANK, RANK), 1)
    return jnp.where(rows == columns, 1.0, 0.0).astype(jnp.float32)


def trace(matrix):
    size = matrix.shape[0]
    rows = lax.broadcasted_iota(jnp.int32, (size, size), 0)
    columns = lax.broadcasted_iota(jnp.int32, (size, size), 1)
    kept = jnp.where(rows == columns, matrix, 0.0)
    return jnp.sum(jnp.sum(kept, axis=1, keepdims=True), axis=0, keepdims=True)


def factorize(matrices, work, inverse=True):
    count = len(matrices)
    for k in range(count):
        work[k, :, :RANK] = matrices[k]
    lane = lax.broadcasted_iota(jnp.int32, (8, RANK), 1)
    sub = lax.broadcasted_iota(jnp.int32, (8, RANK), 0)
    rows = lax.broadcasted_iota(jnp.int32, (RANK, RANK), 0)
    cols_i = lax.broadcasted_iota(jnp.int32, (RANK, RANK), 1)
    groups = BLOCK // 8

    def step(index, carry):
        first = pl.multiple_of(index * BLOCK, BLOCK)
        here = lane - first
        left = [[work[k, pl.ds(first + 8 * g, 8), :RANK] for g in range(groups)] for k in range(count)]
        for start in range(0, BLOCK, SUB):
            active = range(start // 8, groups)
            columns = [
                [
                    {
                        g: jnp.broadcast_to(
                            jnp.sum(jnp.where(here == start + c, left[k][g], 0.0), axis=1, keepdims=True),
                            (8, RANK),
                        )
                        for g in active
                        if 8 * g + 7 >= start + c
                    }
                    for c in range(SUB)
                ]
                for k in range(count)
            ]
            if inverse:
                inside = (here >= start) & (here < start + SUB)
                for k in range(count):
                    for g in active:
                        unit = jnp.where(here == sub + 8 * g, 1.0, 0.0)
                        left[k][g] = jnp.where(inside, unit, left[k][g])
            for i in range(0, SUB, 2):
                at, row = divmod(start + i, 8)
                for k in range(count):
                    one, two = columns[k][i], columns[k][i + 1]
                    a = one[at][row : row + 1]
                    b = one[at][row + 1 : row + 2]
                    c = two[at][row + 1 : row + 2]
                    det = a * c - b * b
                    scale = lax.rsqrt(det)
                    inv = scale * scale
                    root = lax.rsqrt(a)
                    up, down = left[k][at][row : row + 1], left[k][at][row + 1 : row + 2]
                    for g in active:
                        if g < at or (g == at and row == 6):
                            continue
                        u = (c * one[g] - b * two[g]) * inv
                        v = (a * two[g] - b * one[g]) * inv
                        for j in range(i + 2, SUB):
                            if 8 * g + 7 >= start + j:
                                to, spot = divmod(start + j, 8)
                                columns[k][j][g] = columns[k][j][g] - (
                                    u * one[to][spot : spot + 1] + v * two[to][spot : spot + 1]
                                )
                        if g == at:
                            u = jnp.where(sub > row + 1, u, 0.0)
                            v = jnp.where(sub > row + 1, v, 0.0)
                        left[k][g] = left[k][g] - (u * up + v * down)
                    down = (a * down - b * up) * (root * scale)
                    left[k][at] = jnp.where(
                        sub == row, up * root, jnp.where(sub == row + 1, down, left[k][at])
                    )
        for k in range(count):
            if inverse:
                for g in range(SUB // 8):
                    left[k][g] = jnp.where((here >= SUB) & (here < BLOCK), 0.0, left[k][g])
            for g in range(groups):
                work[k, pl.ds(first + 8 * g, 8), :RANK] = left[k][g]

        @pl.when(index < RANK // BLOCK - 1)
        def _():
            for k in range(count):
                whole = jnp.concatenate(left[k], axis=0)
                wide = lax.broadcasted_iota(jnp.int32, (BLOCK, RANK), 1)
                a, b, c = split_3(whole)
                h, m, l = (jnp.where(wide >= first + BLOCK, part.astype(jnp.float32), 0.0) for part in (a, b, c))
                lhs = jnp.concatenate([h, h, m, m, h, l, jnp.zeros((2 * BLOCK, RANK), jnp.float32)], axis=0)
                lhs = lhs.T.astype(jnp.bfloat16)
                rhs = jnp.concatenate([a, b, a, b, c, a, jnp.zeros((2 * BLOCK, RANK), jnp.bfloat16)], axis=0)
                update = jnp.dot(lhs, rhs, preferred_element_type=jnp.float32)
                old = work[k, :, :RANK]
                if inverse:
                    inside = (cols_i >= first) & (cols_i < first + BLOCK) & (rows >= first + BLOCK)
                    old = jnp.where(inside, 0.0, old)
                work[k, :, :RANK] = old - update
        return carry

    lax.fori_loop(0, RANK // BLOCK, step, 0)
    if inverse:
        return [jnp.where(cols_i <= rows, work[k, :, :RANK], 0.0) for k in range(count)]
    return [jnp.where(cols_i >= rows, work[k, :, :RANK], 0.0) for k in range(count)]


def reduce_grams(grams, work):
    scaled = [gram * (1.0 / trace(gram)) for gram in grams]
    images = [(gram[:RANK, :] + gram[RANK:, :]) * 0.7071067811865476 for gram in scaled]
    inverses = factorize([mm_t(image, image) for image in images], work)
    bases = [mm(inverse, image) for inverse, image in zip(inverses, images)]
    quotients = [mm_t(mm(basis, gram), basis) for basis, gram in zip(bases, scaled)]
    tails = [(trace(gram) - trace(quotient)) / RANK for gram, quotient in zip(scaled, quotients)]
    uppers = factorize(quotients, work, False)
    turned = [mm(upper, basis) for upper, basis in zip(uppers, bases)]
    inverses = factorize([mm_t(u, u) + tail * eye() for u, tail in zip(uppers, tails)], work)
    out = []
    for inverse, turn, gram in zip(inverses, turned, grams):
        mixing = mm(inverse, turn)
        out.append((mixing, mm_t(mm(mixing, gram), mixing)))
    return out


def kernel(levels, feats, ridge_ref, rows_ref, out_ref, *scratch):
    work, tree, prefix, partner = scratch[:4]
    slab_slots = scratch[4]
    level_slots = scratch[5 : 5 + levels]
    last_slots = scratch[5 + levels]
    send_sem, recv_sem, pair_send, pair_recv = scratch[6 + levels :]
    seq = lax.axis_index("seq")
    feat = lax.axis_index("feat")
    width = rows_ref.shape[1]

    def bit_of(level):
        return lax.rem(seq // (1 << level), 2)

    def sibling(level):
        return seq + (1 << level) - 2 * (1 << level) * bit_of(level)

    barrier = pltpu.get_barrier_semaphore()
    for offset in range(1, feats):
        pl.semaphore_signal(
            barrier, inc=1, device_id=(seq, lax.rem(feat + offset, feats)), device_id_type=MESH
        )
    for level in range(levels):
        pl.semaphore_signal(
            barrier, inc=1, device_id=(sibling(level), feat), device_id_type=MESH
        )
    pl.semaphore_wait(barrier, feats - 1 + levels)

    def send_sum(slots, phase):
        copies = []
        for offset in range(1, feats):
            copy = pltpu.make_async_remote_copy(
                src_ref=slots.at[feat],
                dst_ref=slots.at[feat],
                send_sem=send_sem.at[phase, offset],
                recv_sem=recv_sem.at[phase, offset],
                device_id=(seq, lax.rem(feat + offset, feats)),
                device_id_type=MESH,
            )
            copy.start()
            copies.append(copy)
        return copies

    def finish_sum(slots, copies):
        for copy in copies:
            copy.wait()
        total = slots[0]
        for index in range(1, feats):
            total = total + slots[index]
        return total

    def fetch(level):
        for index, hop in enumerate(range(level, -1, -1)):
            source = tree if hop == level else partner
            bits = hop if hop == level else hop + 1
            size = RANK >> bits
            first = 0
            for bit in range(bits):
                first = first + bit_of(bit) * (RANK >> (bit + 1))
            span = pl.ds(pl.multiple_of(first, size), size) if bits else pl.ds(0, RANK)
            copy = pltpu.make_async_remote_copy(
                src_ref=source.at[level, span],
                dst_ref=partner.at[level, span],
                send_sem=pair_send.at[level, index],
                recv_sem=pair_recv.at[level, index],
                device_id=(sibling(hop), feat),
                device_id_type=MESH,
            )
            copy.start()
            copy.wait()

    rows = rows_ref[...]
    slab_slots[feat] = lax.dot_general(
        rows, rows, (((1,), (1,)), ((), ())), preferred_element_type=jnp.float32
    )
    gram = finish_sum(slab_slots, send_sum(slab_slots, 0))
    ((mixing, own_gram),) = reduce_grams([gram], work)
    h, m, l = split_3(mixing)
    sketch = (
        jnp.dot(l, rows, preferred_element_type=jnp.float32)
        + jnp.dot(m, rows, preferred_element_type=jnp.float32)
        + jnp.dot(h, rows, preferred_element_type=jnp.float32)
    )
    tree[0, :, :width] = sketch
    tree[0, :, width:] = own_gram
    prefix[...] = sketch
    prefix_gram = own_gram

    for level in range(levels):
        fetch(level)
        slots = level_slots[level]
        with_prefix = level > 0
        with_tree = level + 1 < levels or level == 0
        lefts = []
        if with_tree:
            lefts.append((tree.at[level, :, :width], tree[level, :, width:]))
        if with_prefix:
            lefts.append((prefix, prefix_gram))
        for index, (left, _) in enumerate(lefts):
            slots[feat, index * RANK : (index + 1) * RANK, :] = mm_t(
                left[...], partner[level, :, :width]
            )
        crosses = finish_sum(slots, send_sum(slots, 1 + level))
        other = partner[level, :, width:]
        stacked = []
        for index, (_, left_gram) in enumerate(lefts):
            cross = crosses[index * RANK : (index + 1) * RANK]
            stacked.append(
                jnp.concatenate(
                    [
                        jnp.concatenate([left_gram, cross], 1),
                        jnp.concatenate([cross.T, other], 1),
                    ],
                    0,
                )
            )
        results = reduce_grams(stacked, work)
        merged = []
        for (left, _), (mixing, new_gram) in zip(lefts, results):
            merged.append(
                (mm(mixing[:, :RANK], left[...]) + mm(mixing[:, RANK:], partner[level, :, :width]), new_gram)
            )
        keep = bit_of(level) == 1
        prefix[...] = jnp.where(keep, merged[-1][0], prefix[...])
        prefix_gram = jnp.where(keep, merged[-1][1], prefix_gram)
        if level + 1 < levels:
            tree[level + 1, :, :width] = merged[0][0]
            tree[level + 1, :, width:] = merged[0][1]

    ridge = ridge_ref[0, 0]
    seen_rows = ((seq + 1) * rows_ref.shape[0]).astype(jnp.float32)
    seen = jnp.full((1, 1), seen_rows * ridge, jnp.float32)
    half_basis = (prefix[...] * lax.rsqrt(seen)).astype(jnp.bfloat16)
    last_slots[feat] = lax.dot_general(
        rows, half_basis, (((1,), (1,)), ((), ())), preferred_element_type=jnp.float32
    )
    copies = send_sum(last_slots, 1 + levels)
    shifted = eye() + prefix_gram / seen
    norm = jnp.sqrt(
        jnp.sum(jnp.sum(shifted * shifted, axis=1, keepdims=True), axis=0, keepdims=True)
    )

    work[0, :, :RANK] = shifted / norm
    work[0, :, RANK:] = eye()

    def root_step(index, carry):
        current, other = work[0, :, :RANK], work[0, :, RANK:]
        middle = 1.5 * eye() - 0.5 * mm(other, current)
        work[0, :, :RANK] = mm(current, middle)
        work[0, :, RANK:] = mm(middle, other)
        return carry

    lax.fori_loop(0, ROOT_STEPS, root_step, 0)
    current = work[0, :, :RANK]
    total_gram = shifted + current * jnp.sqrt(norm)
    total_gram = 0.5 * (total_gram + total_gram.T)
    (inverse,) = factorize([total_gram], work)
    projection = finish_sum(last_slots, copies)
    coefficients = mm(mm_t(projection, inverse), inverse).astype(jnp.bfloat16)
    restored = jnp.dot(coefficients, half_basis, preferred_element_type=jnp.float32)
    out_ref[...] = (
        (rows.astype(jnp.float32) - restored) * lax.rsqrt(jnp.full((1, 1), ridge, jnp.float32))
    ).astype(jnp.bfloat16)


def on_device(activations, ridge_scale):
    tokens, width = activations.shape
    feats = lax.axis_size("feat")
    levels = lax.axis_size("seq").bit_length() - 1
    wide = (RANK, width)
    f32 = jnp.float32
    scratch = [
        pltpu.VMEM((2, RANK, 2 * RANK), f32),
        pltpu.VMEM((levels, RANK, width + RANK), f32),
        pltpu.VMEM(wide, f32),
        pltpu.VMEM((levels, RANK, width + RANK), f32),
        pltpu.VMEM((feats, tokens, tokens), f32),
    ]
    for level in range(levels):
        count = 2 if 0 < level < levels - 1 else 1
        scratch.append(pltpu.VMEM((feats, count * RANK, RANK), f32))
    scratch.append(pltpu.VMEM((feats, tokens, RANK), f32))
    scratch += [
        pltpu.SemaphoreType.DMA((levels + 2, feats)),
        pltpu.SemaphoreType.DMA((levels + 2, feats)),
        pltpu.SemaphoreType.DMA((levels, levels)),
        pltpu.SemaphoreType.DMA((levels, levels)),
    ]
    return pl.pallas_call(
        functools.partial(kernel, levels, feats),
        out_shape=jax.ShapeDtypeStruct(activations.shape, activations.dtype),
        in_specs=[
            pl.BlockSpec(memory_space=pltpu.SMEM),
            pl.BlockSpec(memory_space=pltpu.VMEM),
        ],
        out_specs=pl.BlockSpec(memory_space=pltpu.VMEM),
        scratch_shapes=scratch,
        compiler_params=pltpu.CompilerParams(
            collective_id=0, has_side_effects=True, vmem_limit_bytes=60 * 1024 * 1024
        ),
    )(ridge_scale.reshape(1, 1), activations)


def solution(mesh):
    placed = (P("seq", "feat"), P())
    return jax.shard_map(
        on_device, mesh=mesh, in_specs=placed, out_specs=P("seq", "feat"), check_vma=False
    )
```

```python
import functools

import jax
import jax.numpy as jnp
from jax import lax
from jax.experimental import pallas as pl
from jax.experimental.pallas import tpu as pltpu
from jax.sharding import PartitionSpec as P

RANK = 128
ROOT_STEPS = 12
BLOCK = 32
SUB = 16
MESH = pl.DeviceIdType.MESH
HIGHEST = lax.Precision.HIGHEST


def mm(a, b):
    return jnp.dot(a, b, precision=HIGHEST, preferred_element_type=jnp.float32)


def mm_t(a, b):
    return lax.dot_general(
        a, b, (((1,), (1,)), ((), ())), precision=HIGHEST, preferred_element_type=jnp.float32
    )


def split_3(x):
    high = x.astype(jnp.bfloat16)
    rest = x - high.astype(jnp.float32)
    middle = rest.astype(jnp.bfloat16)
    low = (rest - middle.astype(jnp.float32)).astype(jnp.bfloat16)
    return high, middle, low


def eye():
    rows = lax.broadcasted_iota(jnp.int32, (RANK, RANK), 0)
    columns = lax.broadcasted_iota(jnp.int32, (RANK, RANK), 1)
    return jnp.where(rows == columns, 1.0, 0.0).astype(jnp.float32)


def trace(matrix):
    size = matrix.shape[0]
    rows = lax.broadcasted_iota(jnp.int32, (size, size), 0)
    columns = lax.broadcasted_iota(jnp.int32, (size, size), 1)
    kept = jnp.where(rows == columns, matrix, 0.0)
    return jnp.sum(jnp.sum(kept, axis=1, keepdims=True), axis=0, keepdims=True)


def factorize(matrices, work, inverse=True):
    count = len(matrices)
    for k in range(count):
        work[k, :, :RANK] = matrices[k]
    lane = lax.broadcasted_iota(jnp.int32, (8, RANK), 1)
    sub = lax.broadcasted_iota(jnp.int32, (8, RANK), 0)
    rows = lax.broadcasted_iota(jnp.int32, (RANK, RANK), 0)
    cols_i = lax.broadcasted_iota(jnp.int32, (RANK, RANK), 1)
    groups = BLOCK // 8

    def step(index, carry):
        first = pl.multiple_of(index * BLOCK, BLOCK)
        here = lane - first
        left = [[work[k, pl.ds(first + 8 * g, 8), :RANK] for g in range(groups)] for k in range(count)]
        for start in range(0, BLOCK, SUB):
            active = range(start // 8, groups)
            columns = [
                [
                    {
                        g: jnp.broadcast_to(
                            jnp.sum(jnp.where(here == start + c, left[k][g], 0.0), axis=1, keepdims=True),
                            (8, RANK),
                        )
                        for g in active
                        if 8 * g + 7 >= start + c
                    }
                    for c in range(SUB)
                ]
                for k in range(count)
            ]
            if inverse:
                inside = (here >= start) & (here < start + SUB)
                for k in range(count):
                    for g in active:
                        unit = jnp.where(here == sub + 8 * g, 1.0, 0.0)
                        left[k][g] = jnp.where(inside, unit, left[k][g])
            for i in range(0, SUB, 2):
                at, row = divmod(start + i, 8)
                for k in range(count):
                    one, two = columns[k][i], columns[k][i + 1]
                    a = one[at][row : row + 1]
                    b = one[at][row + 1 : row + 2]
                    c = two[at][row + 1 : row + 2]
                    det = a * c - b * b
                    scale = lax.rsqrt(det)
                    inv = scale * scale
                    root = lax.rsqrt(a)
                    up, down = left[k][at][row : row + 1], left[k][at][row + 1 : row + 2]
                    for g in active:
                        if g < at or (g == at and row == 6):
                            continue
                        u = (c * one[g] - b * two[g]) * inv
                        v = (a * two[g] - b * one[g]) * inv
                        for j in range(i + 2, SUB):
                            if 8 * g + 7 >= start + j:
                                to, spot = divmod(start + j, 8)
                                columns[k][j][g] = columns[k][j][g] - (
                                    u * one[to][spot : spot + 1] + v * two[to][spot : spot + 1]
                                )
                        if g == at:
                            u = jnp.where(sub > row + 1, u, 0.0)
                            v = jnp.where(sub > row + 1, v, 0.0)
                        left[k][g] = left[k][g] - (u * up + v * down)
                    down = (a * down - b * up) * (root * scale)
                    left[k][at] = jnp.where(
                        sub == row, up * root, jnp.where(sub == row + 1, down, left[k][at])
                    )
        for k in range(count):
            if inverse:
                for g in range(SUB // 8):
                    left[k][g] = jnp.where((here >= SUB) & (here < BLOCK), 0.0, left[k][g])
            for g in range(groups):
                work[k, pl.ds(first + 8 * g, 8), :RANK] = left[k][g]

        @pl.when(index < RANK // BLOCK - 1)
        def _():
            for k in range(count):
                whole = jnp.concatenate(left[k], axis=0)
                wide = lax.broadcasted_iota(jnp.int32, (BLOCK, RANK), 1)
                a, b, c = split_3(whole)
                h, m, l = (jnp.where(wide >= first + BLOCK, part.astype(jnp.float32), 0.0) for part in (a, b, c))
                lhs = jnp.concatenate([h, h, m, m, h, l, jnp.zeros((2 * BLOCK, RANK), jnp.float32)], axis=0)
                lhs = lhs.T.astype(jnp.bfloat16)
                rhs = jnp.concatenate([a, b, a, b, c, a, jnp.zeros((2 * BLOCK, RANK), jnp.bfloat16)], axis=0)
                update = jnp.dot(lhs, rhs, preferred_element_type=jnp.float32)
                old = work[k, :, :RANK]
                if inverse:
                    inside = (cols_i >= first) & (cols_i < first + BLOCK) & (rows >= first + BLOCK)
                    old = jnp.where(inside, 0.0, old)
                work[k, :, :RANK] = old - update
        return carry

    lax.fori_loop(0, RANK // BLOCK, step, 0)
    if inverse:
        return [jnp.where(cols_i <= rows, work[k, :, :RANK], 0.0) for k in range(count)]
    return [jnp.where(cols_i >= rows, work[k, :, :RANK], 0.0) for k in range(count)]


def reduce_grams(grams, work, between=None):
    scaled = [gram * (1.0 / trace(gram)) for gram in grams]
    images = [(gram[:RANK, :] + gram[RANK:, :]) * 0.7071067811865476 for gram in scaled]
    inverses = factorize([mm_t(image, image) for image in images], work)
    if between is not None:
        between()
    bases = [mm(inverse, image) for inverse, image in zip(inverses, images)]
    quotients = [mm_t(mm(basis, gram), basis) for basis, gram in zip(bases, scaled)]
    tails = [(trace(gram) - trace(quotient)) / RANK for gram, quotient in zip(scaled, quotients)]
    uppers = factorize(quotients, work, False)
    turned = [mm(upper, basis) for upper, basis in zip(uppers, bases)]
    inverses = factorize([mm_t(u, u) + tail * eye() for u, tail in zip(uppers, tails)], work)
    out = []
    for inverse, turn, gram in zip(inverses, turned, grams):
        mixing = mm(inverse, turn)
        out.append((mixing, mm_t(mm(mixing, gram), mixing)))
    return out


def mix_rows(mixing, rows):
    h, m, l = split_3(mixing)
    return (
        jnp.dot(l, rows, preferred_element_type=jnp.float32)
        + jnp.dot(m, rows, preferred_element_type=jnp.float32)
        + jnp.dot(h, rows, preferred_element_type=jnp.float32)
    )


def stack(first, cross, last):
    return jnp.concatenate(
        [jnp.concatenate([first, cross], 1), jnp.concatenate([cross.T, last], 1)], 0
    )


def fold(gram):
    rows = lax.broadcasted_iota(jnp.int32, (RANK, RANK), 0)
    columns = lax.broadcasted_iota(jnp.int32, (RANK, RANK), 1)
    first, last = gram[:RANK, :RANK], gram[RANK:, RANK:]
    both = jnp.where(columns <= rows, first, last)
    diagonal = jnp.sum(jnp.where(columns == rows, last, 0.0), axis=0, keepdims=True)
    return both, gram[:RANK, RANK:], jnp.broadcast_to(diagonal, (8, RANK))


def unfold(both, cross, diagonal):
    rows = lax.broadcasted_iota(jnp.int32, (RANK, RANK), 0)
    columns = lax.broadcasted_iota(jnp.int32, (RANK, RANK), 1)
    turned = both.T
    first = jnp.where(columns <= rows, both, turned)
    last = jnp.where(columns > rows, both, jnp.where(columns < rows, turned, diagonal))
    return stack(first, cross, last)


def kernel(levels, feats, names, ridge_ref, rows_ref, out_ref, *scratch):
    at = dict(zip(names, scratch))
    work, tree, partner, prefix = at["work"], at["tree"], at["partner"], at["prefix"]
    prefix_gram, lower = at["prefix_gram"], at["lower"]
    send_sem, recv_sem = at["send_sem"], at["recv_sem"]
    pair_send, pair_recv = at["pair_send"], at["pair_recv"]
    core_send, core_recv = at["core_send"], at["core_recv"]
    up_send, up_recv = at["up_send"], at["up_recv"]
    share_send, share_recv = at["share_send"], at["share_recv"]
    seq = lax.axis_index("seq")
    feat = lax.axis_index("feat")
    width = rows_ref.shape[1]
    top, under = levels - 1, levels - 2

    def bit_of(level):
        return lax.rem(seq // (1 << level), 2)

    def flipped(level):
        return (1 << level) - 2 * (1 << level) * bit_of(level)

    def sibling(level):
        return seq + flipped(level)

    cousin = seq + flipped(top) + flipped(under)
    upper = bit_of(top) == 1
    far = bit_of(under) == 1
    is_ll = (bit_of(top) == 0) & (bit_of(under) == 0)
    is_lr = (bit_of(top) == 0) & (bit_of(under) == 1)
    is_ul = (bit_of(top) == 1) & (bit_of(under) == 0)
    is_ur = (bit_of(top) == 1) & (bit_of(under) == 1)

    barrier = pltpu.get_barrier_semaphore()
    for offset in range(1, feats):
        pl.semaphore_signal(
            barrier, inc=1, device_id=(seq, lax.rem(feat + offset, feats)), device_id_type=MESH
        )
    for other in [sibling(level) for level in range(levels)] + [cousin]:
        pl.semaphore_signal(barrier, inc=1, device_id=(other, feat), device_id_type=MESH)
    rows = rows_ref[...]
    at["own_rows"][...] = rows.astype(jnp.float32)
    local = lax.dot_general(
        rows, rows, (((1,), (1,)), ((), ())), preferred_element_type=jnp.float32
    )
    pl.semaphore_wait(barrier, feats + levels)

    def remote(src, dst, sends, recvs, other):
        return pltpu.make_async_remote_copy(
            src_ref=src, dst_ref=dst, send_sem=sends, recv_sem=recvs,
            device_id=(other, feat), device_id_type=MESH,
        )

    def send_sum(slots, phase):
        copies = []
        for offset in range(1, feats):
            copy = pltpu.make_async_remote_copy(
                src_ref=slots.at[feat],
                dst_ref=slots.at[feat],
                send_sem=send_sem.at[phase, offset],
                recv_sem=recv_sem.at[phase, offset],
                device_id=(seq, lax.rem(feat + offset, feats)),
                device_id_type=MESH,
            )
            copy.start()
            copies.append(copy)
        return copies

    def finish_sum(slots, copies):
        for copy in copies:
            copy.wait()
        total = slots[0]
        for index in range(1, feats):
            total = total + slots[index]
        return total

    def part(bits):
        size = RANK >> bits
        first = 0
        for bit in range(bits):
            first = first + bit_of(bit) * (RANK >> (bit + 1))
        return pl.ds(pl.multiple_of(first, size), size) if bits else pl.ds(0, RANK)

    def fetch(level):
        for index, hop in enumerate(range(level, -1, -1)):
            source = tree if hop == level else partner
            span = part(hop if hop == level else hop + 1)
            copy = remote(
                source.at[level, span], partner.at[level, span],
                pair_send.at[level, index], pair_recv.at[level, index], sibling(hop),
            )
            copy.start()
            copy.wait()

    parity = bit_of(0)
    rows_copy = remote(
        at["own_rows"], at["other_rows"], core_send.at[0], core_recv.at[0], sibling(0)
    )
    rows_copy.start()
    slab_slots, cross_slots, cross_full = at["slab_slots"], at["cross_slots"], at["cross_full"]
    both, between, diagonal = fold(local)
    slab_slots[feat, :RANK] = both
    slab_slots[feat, RANK : 2 * RANK] = between
    slab_slots[feat, 2 * RANK :] = diagonal
    slab_copies = send_sum(slab_slots, 0)
    rows_copy.wait()
    other_rows = at["other_rows"][...].astype(jnp.bfloat16)
    half = jnp.where(
        parity == 0, at["own_rows"][:RANK], at["other_rows"][RANK:]
    ).astype(jnp.bfloat16)
    odd_rows = jnp.where(parity == 0, at["other_rows"][...], at["own_rows"][...]).astype(jnp.bfloat16)
    cross_slots[feat] = lax.dot_general(
        half, odd_rows, (((1,), (1,)), ((), ())), preferred_element_type=jnp.float32
    )
    cross_copies = send_sum(cross_slots, 1)
    packed = finish_sum(slab_slots, slab_copies)
    gram = unfold(packed[:RANK], packed[RANK : 2 * RANK], packed[2 * RANK : 2 * RANK + 1])

    share = remote(
        cross_full.at[parity], cross_full.at[parity], core_send.at[1], core_recv.at[1], sibling(0)
    )

    def share_cross():
        cross_full[parity] = finish_sum(cross_slots, cross_copies)
        share.start()

    ((mixing, own_gram),) = reduce_grams([gram], work, share_cross)
    mixes = at["mixes"]
    mixes[parity, :, : 2 * RANK] = mixing
    mixes[parity, :, 2 * RANK :] = own_gram
    swap = remote(mixes.at[parity], mixes.at[parity], core_send.at[2], core_recv.at[2], sibling(0))
    swap.start()
    prefix[...] = mix_rows(mixing, rows)
    share.wait()
    swap.wait()
    even, odd = mixes[0, :, : 2 * RANK], mixes[1, :, : 2 * RANK]
    crossed = jnp.concatenate([cross_full[0], cross_full[1]], 0)
    crossed = mm_t(mm(even, crossed), odd)
    ((mixing, new_gram),) = reduce_grams(
        [stack(mixes[0, :, 2 * RANK :], crossed, mixes[1, :, 2 * RANK :])], work
    )
    even, odd = mm(mixing[:, :RANK], even), mm(mixing[:, RANK:], odd)
    block = mix_rows(jnp.where(parity == 0, even, odd), rows) + mix_rows(
        jnp.where(parity == 0, odd, even), other_rows
    )
    tree[1, :, :width] = block
    tree[1, :, width:] = new_gram
    prefix[...] = jnp.where(parity == 1, block, prefix[...])
    prefix_gram[...] = jnp.where(parity == 1, new_gram, own_gram)

    mine = part(under)
    size = RANK >> under
    near = [pl.ds(pl.multiple_of(mine.start + piece * (size // 2), size // 2), size // 2) for piece in range(2)]

    def lift(index, source, span, slot, other):
        return remote(
            source, lower.at[slot, span], up_send.at[index], up_recv.at[index], other
        )

    send_right = lift(0, tree.at[under, mine, pl.ds(0, width)], mine, 1, cousin)
    send_left = [
        lift(1 + piece, partner.at[under, near[piece], pl.ds(0, width)], near[piece], 0, cousin)
        for piece in range(2)
    ]
    pass_right = lift(3, lower.at[1, mine], mine, 1, sibling(under))
    pass_left = [
        lift(4 + piece, lower.at[0, near[piece]], near[piece], 0, sibling(under))
        for piece in range(2)
    ]

    for level in range(1, top):
        last = level == under
        if last:
            @pl.when(is_lr)
            def _():
                send_right.start()

        fetch(level)
        if last:
            @pl.when(is_lr)
            def _():
                for copy in send_left:
                    copy.start()

            @pl.when(is_ul)
            def _():
                send_right.wait_recv()
                pass_right.start()

        other = partner[level, :, :width]
        other_gram = partner[level, :, width:]
        lefts = [(tree[level, :, :width], tree[level, :, width:]), (prefix[...], prefix_gram[...])]
        if last:
            full = bit_of(0)
            for bit in range(1, level):
                full = full * bit_of(bit)
            own = far & (full == 0)
            lefts = [tuple(jnp.where(own, mine_, tree_) for tree_, mine_ in zip(*lefts))]
        slots = at["level_slots"] if last else at["twin_slots"].at[level - 1]
        for index, (left, _) in enumerate(lefts):
            slots[feat, index * RANK : (index + 1) * RANK, :] = mm_t(left, other)
        crosses = finish_sum(slots, send_sum(slots, 1 + level))

        def pass_on():
            @pl.when(is_ul)
            def _():
                send_left[1].wait_recv()
                pass_left[1].start()

        if last:
            @pl.when(is_ul)
            def _():
                send_left[0].wait_recv()
                pass_left[0].start()

        results = reduce_grams(
            [
                stack(left_gram, crosses[index * RANK : (index + 1) * RANK], other_gram)
                for index, (_, left_gram) in enumerate(lefts)
            ],
            work,
            pass_on if last else None,
        )
        if last:
            sent, got = at["top_sent"], at["top_got"]
            sent[:, : 2 * RANK] = results[0][0]
            sent[:, 2 * RANK :] = results[0][1]
            above = [
                remote(sent, got, up_send.at[6], up_recv.at[6], seq + flipped(top) + flipped(under)),
                remote(sent, got, up_send.at[7], up_recv.at[6], seq + flipped(top)),
            ]

            @pl.when(is_ll)
            def _():
                for copy in above:
                    copy.start()

            @pl.when(is_ur)
            def _():
                pass_right.wait_recv()
                for copy in pass_left:
                    copy.wait_recv()

            shares = []
            for hop in range(under - 1, -1, -1):
                shares.append(
                    [
                        remote(
                            lower.at[slot, part(hop + 1)], lower.at[slot, part(hop + 1)],
                            share_send.at[slot, hop], share_recv.at[slot, hop], sibling(hop),
                        )
                        for slot in range(2)
                    ]
                )

            @pl.when(upper)
            def _():
                for copy in shares[0]:
                    copy.start()

        merged = [
            (mm(mixing[:, :RANK], left) + mm(mixing[:, RANK:], other), new_gram)
            for (left, _), (mixing, new_gram) in zip(lefts, results)
        ]
        keep = bit_of(level) == 1
        prefix[...] = jnp.where(keep, merged[-1][0], prefix[...])
        prefix_gram[...] = jnp.where(keep, merged[-1][1], prefix_gram[...])
        if not last:
            tree[level + 1, :, :width] = merged[0][0]
            tree[level + 1, :, width:] = merged[0][1]

    @pl.when(is_lr)
    def _():
        send_right.wait_send()
        for copy in send_left:
            copy.wait_send()

    @pl.when(is_ll)
    def _():
        for copy in above:
            copy.wait_send()

    @pl.when(is_ul)
    def _():
        pass_right.wait_send()
        for copy in pass_left:
            copy.wait_send()

    @pl.when(upper)
    def _():
        for index, pair in enumerate(shares):
            if index:
                for copy in pair:
                    copy.start()
            for copy in pair:
                copy.wait()
        slots = at["top_slots"]
        for slot in range(2):
            slots[feat, slot * RANK : (slot + 1) * RANK, :] = mm_t(lower[slot], prefix[...])
        copies = send_sum(slots, 1 + top)
        above[0].wait_recv()
        got = at["top_got"]
        mixed = got[:, : 2 * RANK]
        crossed = mm(mixed, finish_sum(slots, copies))
        ((mixing, new_gram),) = reduce_grams(
            [stack(got[:, 2 * RANK :], crossed, prefix_gram[...])], work
        )
        mixed = mm(mixing[:, :RANK], mixed)
        prefix[...] = (
            mm(mixed[:, :RANK], lower[0])
            + mm(mixed[:, RANK:], lower[1])
            + mm(mixing[:, RANK:], prefix[...])
        )
        prefix_gram[...] = new_gram

    ridge = ridge_ref[0, 0]
    seen_rows = ((seq + 1) * rows_ref.shape[0]).astype(jnp.float32)
    seen = jnp.full((1, 1), seen_rows * ridge, jnp.float32)
    half_basis = (prefix[...] * lax.rsqrt(seen)).astype(jnp.bfloat16)
    at["last_slots"][feat] = lax.dot_general(
        rows, half_basis, (((1,), (1,)), ((), ())), preferred_element_type=jnp.float32
    )
    copies = send_sum(at["last_slots"], 1 + levels)
    shifted = eye() + prefix_gram[...] / seen
    norm = jnp.sqrt(
        jnp.sum(jnp.sum(shifted * shifted, axis=1, keepdims=True), axis=0, keepdims=True)
    )

    work[0, :, :RANK] = shifted / norm
    work[0, :, RANK:] = eye()

    def root_step(index, carry):
        current, other = work[0, :, :RANK], work[0, :, RANK:]
        middle = 1.5 * eye() - 0.5 * mm(other, current)
        work[0, :, :RANK] = mm(current, middle)
        work[0, :, RANK:] = mm(middle, other)
        return carry

    lax.fori_loop(0, ROOT_STEPS, root_step, 0)
    current = work[0, :, :RANK]
    total_gram = shifted + current * jnp.sqrt(norm)
    total_gram = 0.5 * (total_gram + total_gram.T)
    (inverse,) = factorize([total_gram], work)
    projection = finish_sum(at["last_slots"], copies)
    coefficients = mm(mm_t(projection, inverse), inverse).astype(jnp.bfloat16)
    restored = jnp.dot(coefficients, half_basis, preferred_element_type=jnp.float32)
    out_ref[...] = (
        (rows.astype(jnp.float32) - restored) * lax.rsqrt(jnp.full((1, 1), ridge, jnp.float32))
    ).astype(jnp.bfloat16)


def on_device(activations, ridge_scale):
    tokens, width = activations.shape
    feats = lax.axis_size("feat")
    levels = lax.axis_size("seq").bit_length() - 1
    f32 = jnp.float32
    dma = pltpu.SemaphoreType.DMA
    scratch = dict(
        work=pltpu.VMEM((2, RANK, 2 * RANK), f32),
        tree=pltpu.VMEM((levels - 1, RANK, width + RANK), f32),
        partner=pltpu.VMEM((levels - 1, RANK, width + RANK), f32),
        prefix=pltpu.VMEM((RANK, width), f32),
        prefix_gram=pltpu.VMEM((RANK, RANK), f32),
        lower=pltpu.VMEM((2, RANK, width), f32),
        own_rows=pltpu.VMEM((tokens, width), f32),
        other_rows=pltpu.VMEM((tokens, width), f32),
        slab_slots=pltpu.VMEM((feats, 2 * RANK + 8, RANK), f32),
        cross_slots=pltpu.VMEM((feats, RANK, 2 * RANK), f32),
        cross_full=pltpu.VMEM((2, RANK, 2 * RANK), f32),
        mixes=pltpu.VMEM((2, RANK, 3 * RANK), f32),
        level_slots=pltpu.VMEM((feats, RANK, RANK), f32),
        top_sent=pltpu.VMEM((RANK, 3 * RANK), f32),
        top_got=pltpu.VMEM((RANK, 3 * RANK), f32),
        top_slots=pltpu.VMEM((feats, 2 * RANK, RANK), f32),
        last_slots=pltpu.VMEM((feats, tokens, RANK), f32),
        send_sem=dma((levels + 2, feats)),
        recv_sem=dma((levels + 2, feats)),
        pair_send=dma((levels, levels)),
        pair_recv=dma((levels, levels)),
        core_send=dma((3,)),
        core_recv=dma((3,)),
        up_send=dma((8,)),
        up_recv=dma((8,)),
        share_send=dma((2, levels)),
        share_recv=dma((2, levels)),
    )
    if levels > 3:
        scratch["twin_slots"] = pltpu.VMEM((levels - 3, feats, 2 * RANK, RANK), f32)
    return pl.pallas_call(
        functools.partial(kernel, levels, feats, tuple(scratch)),
        out_shape=jax.ShapeDtypeStruct(activations.shape, activations.dtype),
        in_specs=[
            pl.BlockSpec(memory_space=pltpu.SMEM),
            pl.BlockSpec(memory_space=pltpu.VMEM),
        ],
        out_specs=pl.BlockSpec(memory_space=pltpu.VMEM),
        scratch_shapes=list(scratch.values()),
        compiler_params=pltpu.CompilerParams(
            collective_id=0, has_side_effects=True, vmem_limit_bytes=60 * 1024 * 1024
        ),
    )(ridge_scale.reshape(1, 1), activations)


def solution(mesh):
    placed = (P("seq", "feat"), P())
    return jax.shard_map(
        on_device, mesh=mesh, in_specs=placed, out_specs=P("seq", "feat"), check_vma=False
    )
```

```python
import functools

import jax
import jax.numpy as jnp
from jax import lax
from jax.experimental import pallas as pl
from jax.experimental.pallas import tpu as pltpu
from jax.sharding import PartitionSpec as P

RANK = 128
ROOT_STEPS = 12
BLOCK = 32
SUB = 16
MESH = pl.DeviceIdType.MESH
HIGHEST = lax.Precision.HIGHEST


def mm(a, b):
    return jnp.dot(a, b, precision=HIGHEST, preferred_element_type=jnp.float32)


def mm_t(a, b):
    return lax.dot_general(
        a, b, (((1,), (1,)), ((), ())), precision=HIGHEST, preferred_element_type=jnp.float32
    )


def mm_square(a, b):
    a_high, a_middle, a_low = split_3(a)
    b_high, b_middle, b_low = split_3(b)
    pair = jnp.concatenate([b_high, b_middle], 1)
    both = jnp.dot(
        jnp.concatenate([a_high, a_middle], 1),
        jnp.concatenate([pair, pair], 0),
        preferred_element_type=jnp.float32,
    )
    rest = jnp.dot(
        jnp.concatenate([a_high, a_low], 1),
        jnp.concatenate([b_low, b_high], 0),
        preferred_element_type=jnp.float32,
    )
    return both[:, :RANK] + (both[:, RANK:] + rest)


def split_3(x):
    high = x.astype(jnp.bfloat16)
    rest = x - high.astype(jnp.float32)
    middle = rest.astype(jnp.bfloat16)
    low = (rest - middle.astype(jnp.float32)).astype(jnp.bfloat16)
    return high, middle, low


def eye():
    rows = lax.broadcasted_iota(jnp.int32, (RANK, RANK), 0)
    columns = lax.broadcasted_iota(jnp.int32, (RANK, RANK), 1)
    return jnp.where(rows == columns, 1.0, 0.0).astype(jnp.float32)


def trace(matrix):
    size = matrix.shape[0]
    rows = lax.broadcasted_iota(jnp.int32, (size, size), 0)
    columns = lax.broadcasted_iota(jnp.int32, (size, size), 1)
    kept = jnp.where(rows == columns, matrix, 0.0)
    return jnp.sum(jnp.sum(kept, axis=1, keepdims=True), axis=0, keepdims=True)


def factorize(matrices, work, inverse=True):
    count = len(matrices)
    for k in range(count):
        work[k, :, :RANK] = matrices[k]
    lane = lax.broadcasted_iota(jnp.int32, (8, RANK), 1)
    sub = lax.broadcasted_iota(jnp.int32, (8, RANK), 0)
    rows = lax.broadcasted_iota(jnp.int32, (RANK, RANK), 0)
    cols_i = lax.broadcasted_iota(jnp.int32, (RANK, RANK), 1)
    groups = BLOCK // 8

    def step(index, carry):
        first = pl.multiple_of(index * BLOCK, BLOCK)
        here = lane - first
        left = [[work[k, pl.ds(first + 8 * g, 8), :RANK] for g in range(groups)] for k in range(count)]
        for start in range(0, BLOCK, SUB):
            active = range(start // 8, groups)
            columns = [
                [
                    {
                        g: jnp.broadcast_to(
                            jnp.sum(jnp.where(here == start + c, left[k][g], 0.0), axis=1, keepdims=True),
                            (8, RANK),
                        )
                        for g in active
                        if 8 * g + 7 >= start + c
                    }
                    for c in range(SUB)
                ]
                for k in range(count)
            ]
            if inverse:
                inside = (here >= start) & (here < start + SUB)
                for k in range(count):
                    for g in active:
                        unit = jnp.where(here == sub + 8 * g, 1.0, 0.0)
                        left[k][g] = jnp.where(inside, unit, left[k][g])
            for i in range(0, SUB, 2):
                at, row = divmod(start + i, 8)
                for k in range(count):
                    one, two = columns[k][i], columns[k][i + 1]
                    a = one[at][row : row + 1]
                    b = one[at][row + 1 : row + 2]
                    c = two[at][row + 1 : row + 2]
                    det = a * c - b * b
                    scale = lax.rsqrt(det)
                    inv = scale * scale
                    root = lax.rsqrt(a)
                    up, down = left[k][at][row : row + 1], left[k][at][row + 1 : row + 2]
                    for g in active:
                        if g < at or (g == at and row == 6):
                            continue
                        u = (c * one[g] - b * two[g]) * inv
                        v = (a * two[g] - b * one[g]) * inv
                        for j in range(i + 2, SUB):
                            if 8 * g + 7 >= start + j:
                                to, spot = divmod(start + j, 8)
                                columns[k][j][g] = columns[k][j][g] - (
                                    u * one[to][spot : spot + 1] + v * two[to][spot : spot + 1]
                                )
                        if g == at:
                            u = jnp.where(sub > row + 1, u, 0.0)
                            v = jnp.where(sub > row + 1, v, 0.0)
                        left[k][g] = left[k][g] - (u * up + v * down)
                    down = (a * down - b * up) * (root * scale)
                    left[k][at] = jnp.where(
                        sub == row, up * root, jnp.where(sub == row + 1, down, left[k][at])
                    )
        for k in range(count):
            if inverse:
                for g in range(SUB // 8):
                    left[k][g] = jnp.where((here >= SUB) & (here < BLOCK), 0.0, left[k][g])
            for g in range(groups):
                work[k, pl.ds(first + 8 * g, 8), :RANK] = left[k][g]

        @pl.when(index < RANK // BLOCK - 1)
        def _():
            for k in range(count):
                whole = jnp.concatenate(left[k], axis=0)
                wide = lax.broadcasted_iota(jnp.int32, (BLOCK, RANK), 1)
                a, b, c = split_3(whole)
                h, m, l = (jnp.where(wide >= first + BLOCK, part.astype(jnp.float32), 0.0) for part in (a, b, c))
                lhs = jnp.concatenate([h, h, m, m, h, l, jnp.zeros((2 * BLOCK, RANK), jnp.float32)], axis=0)
                lhs = lhs.astype(jnp.bfloat16).T
                rhs = jnp.concatenate([a, b, a, b, c, a, jnp.zeros((2 * BLOCK, RANK), jnp.bfloat16)], axis=0)
                update = jnp.dot(lhs, rhs, preferred_element_type=jnp.float32)
                old = work[k, :, :RANK]
                if inverse:
                    inside = (cols_i >= first) & (cols_i < first + BLOCK) & (rows >= first + BLOCK)
                    old = jnp.where(inside, 0.0, old)
                work[k, :, :RANK] = old - update
        return carry

    lax.fori_loop(0, RANK // BLOCK, step, 0)
    if inverse:
        return [jnp.where(cols_i <= rows, work[k, :, :RANK], 0.0) for k in range(count)]
    return [jnp.where(cols_i >= rows, work[k, :, :RANK], 0.0) for k in range(count)]


def reduce_grams(grams, work, between=None):
    scaled = [gram * (1.0 / trace(gram)) for gram in grams]
    images = [(gram[:RANK, :] + gram[RANK:, :]) * 0.7071067811865476 for gram in scaled]
    inverses = factorize([mm_t(image, image) for image in images], work)
    if between is not None:
        between()
    bases = [mm(inverse, image) for inverse, image in zip(inverses, images)]
    quotients = [mm_t(mm(basis, gram), basis) for basis, gram in zip(bases, scaled)]
    tails = [(trace(gram) - trace(quotient)) / RANK for gram, quotient in zip(scaled, quotients)]
    uppers = factorize(quotients, work, False)
    turned = [mm(upper, basis) for upper, basis in zip(uppers, bases)]
    inverses = factorize([mm_t(u, u) + tail * eye() for u, tail in zip(uppers, tails)], work)
    out = []
    for inverse, turn, gram in zip(inverses, turned, grams):
        mixing = mm(inverse, turn)
        out.append((mixing, mm_t(mm(mixing, gram), mixing)))
    return out


def mix_rows(mixing, rows):
    h, m, l = split_3(mixing)
    return (
        jnp.dot(l, rows, preferred_element_type=jnp.float32)
        + jnp.dot(m, rows, preferred_element_type=jnp.float32)
        + jnp.dot(h, rows, preferred_element_type=jnp.float32)
    )


def split_2(x):
    high = x.astype(jnp.bfloat16)
    return high, (x - high.astype(jnp.float32)).astype(jnp.bfloat16)


def blend(mixing, block):
    a, b = split_2(mixing)
    c, d = split_2(block)
    return (
        jnp.dot(b, c, preferred_element_type=jnp.float32)
        + jnp.dot(a, d, preferred_element_type=jnp.float32)
        + jnp.dot(a, c, preferred_element_type=jnp.float32)
    )


def overlap(first, second):
    a, b = split_2(first)
    c, d = split_2(second)
    dims = (((1,), (1,)), ((), ()))
    return (
        lax.dot_general(b, c, dims, preferred_element_type=jnp.float32)
        + lax.dot_general(a, d, dims, preferred_element_type=jnp.float32)
        + lax.dot_general(a, c, dims, preferred_element_type=jnp.float32)
    )


def stack(first, cross, last):
    return jnp.concatenate(
        [jnp.concatenate([first, cross], 1), jnp.concatenate([cross.T, last], 1)], 0
    )


def fold(gram):
    rows = lax.broadcasted_iota(jnp.int32, (RANK, RANK), 0)
    columns = lax.broadcasted_iota(jnp.int32, (RANK, RANK), 1)
    first, last = gram[:RANK, :RANK], gram[RANK:, RANK:]
    both = jnp.where(columns <= rows, first, last)
    diagonal = jnp.sum(jnp.where(columns == rows, last, 0.0), axis=0, keepdims=True)
    return both, gram[:RANK, RANK:], jnp.broadcast_to(diagonal, (8, RANK))


def unfold(both, cross, diagonal):
    rows = lax.broadcasted_iota(jnp.int32, (RANK, RANK), 0)
    columns = lax.broadcasted_iota(jnp.int32, (RANK, RANK), 1)
    turned = both.T
    first = jnp.where(columns <= rows, both, turned)
    last = jnp.where(columns > rows, both, jnp.where(columns < rows, turned, diagonal))
    return stack(first, cross, last)


def kernel(levels, feats, names, ridge_ref, rows_ref, out_ref, *scratch):
    at = dict(zip(names, scratch))
    work, tree, partner, prefix = at["work"], at["tree"], at["partner"], at["prefix"]
    prefix_gram, lower = at["prefix_gram"], at["lower"]
    send_sem, recv_sem = at["send_sem"], at["recv_sem"]
    pair_send, pair_recv = at["pair_send"], at["pair_recv"]
    core_send, core_recv = at["core_send"], at["core_recv"]
    up_send, up_recv = at["up_send"], at["up_recv"]
    share_send, share_recv = at["share_send"], at["share_recv"]
    seq = lax.axis_index("seq")
    feat = lax.axis_index("feat")
    width = rows_ref.shape[1]
    top, under = levels - 1, levels - 2

    def bit_of(level):
        return lax.rem(seq // (1 << level), 2)

    def flipped(level):
        return (1 << level) - 2 * (1 << level) * bit_of(level)

    def sibling(level):
        return seq + flipped(level)

    cousin = seq + flipped(top) + flipped(under)
    upper = bit_of(top) == 1
    far = bit_of(under) == 1
    is_ll = (bit_of(top) == 0) & (bit_of(under) == 0)
    is_lr = (bit_of(top) == 0) & (bit_of(under) == 1)
    is_ul = (bit_of(top) == 1) & (bit_of(under) == 0)
    is_ur = (bit_of(top) == 1) & (bit_of(under) == 1)

    barrier = pltpu.get_barrier_semaphore()
    for offset in range(1, feats):
        pl.semaphore_signal(
            barrier, inc=1, device_id=(seq, lax.rem(feat + offset, feats)), device_id_type=MESH
        )
    for other in [sibling(level) for level in range(levels)] + [cousin]:
        pl.semaphore_signal(barrier, inc=1, device_id=(other, feat), device_id_type=MESH)
    rows = rows_ref[...]
    at["own_rows"][...] = rows.astype(jnp.float32)
    local = lax.dot_general(
        rows, rows, (((1,), (1,)), ((), ())), preferred_element_type=jnp.float32
    )
    pl.semaphore_wait(barrier, feats + levels)

    def remote(src, dst, sends, recvs, other):
        return pltpu.make_async_remote_copy(
            src_ref=src, dst_ref=dst, send_sem=sends, recv_sem=recvs,
            device_id=(other, feat), device_id_type=MESH,
        )

    def send_sum(slots, phase):
        copies = []
        for offset in range(1, feats):
            copy = pltpu.make_async_remote_copy(
                src_ref=slots.at[feat],
                dst_ref=slots.at[feat],
                send_sem=send_sem.at[phase, offset],
                recv_sem=recv_sem.at[phase, offset],
                device_id=(seq, lax.rem(feat + offset, feats)),
                device_id_type=MESH,
            )
            copy.start()
            copies.append(copy)
        return copies

    def finish_sum(slots, copies):
        for copy in copies:
            copy.wait()
        total = slots[0]
        for index in range(1, feats):
            total = total + slots[index]
        return total

    def part(bits):
        size = RANK >> bits
        first = 0
        for bit in range(bits):
            first = first + bit_of(bit) * (RANK >> (bit + 1))
        return pl.ds(pl.multiple_of(first, size), size) if bits else pl.ds(0, RANK)

    def fetch(level):
        for index, hop in enumerate(range(level, -1, -1)):
            source = tree if hop == level else partner
            span = part(hop if hop == level else hop + 1)
            copy = remote(
                source.at[level, span], partner.at[level, span],
                pair_send.at[level, index], pair_recv.at[level, index], sibling(hop),
            )
            copy.start()
            copy.wait()

    parity = bit_of(0)
    rows_copy = remote(
        at["own_rows"], at["other_rows"], core_send.at[0], core_recv.at[0], sibling(0)
    )
    rows_copy.start()
    far_rows = at["far_rows"]
    pieces = far_rows.shape[1] // at["far_send"].shape[1]
    far_copies, far_shares = [], []
    for piece in range(at["far_send"].shape[1]):
        span = pl.ds(piece * pieces, pieces)
        far_copies.append(
            remote(
                at["own_rows"].at[span], far_rows.at[parity, span],
                at["far_send"].at[0, piece], at["far_recv"].at[0, piece], sibling(1),
            )
        )
        far_shares.append(
            remote(
                far_rows.at[parity, span], far_rows.at[parity, span],
                at["far_send"].at[1, piece], at["far_recv"].at[1, piece], sibling(0),
            )
        )
    for copy in far_copies:
        copy.start()

    def share_far(piece):
        far_copies[piece].wait()
        far_shares[piece].start()

    slab_slots, cross_slots, cross_full = at["slab_slots"], at["cross_slots"], at["cross_full"]
    both, between, diagonal = fold(local)
    slab_slots[feat, :RANK] = both
    slab_slots[feat, RANK : 2 * RANK] = between
    slab_slots[feat, 2 * RANK :] = diagonal
    slab_copies = send_sum(slab_slots, 0)
    rows_copy.wait()
    other_rows = at["other_rows"][...].astype(jnp.bfloat16)
    half = jnp.where(
        parity == 0, at["own_rows"][:RANK], at["other_rows"][RANK:]
    ).astype(jnp.bfloat16)
    odd_rows = jnp.where(parity == 0, at["other_rows"][...], at["own_rows"][...]).astype(jnp.bfloat16)
    cross_slots[feat] = lax.dot_general(
        half, odd_rows, (((1,), (1,)), ((), ())), preferred_element_type=jnp.float32
    )
    cross_copies = send_sum(cross_slots, 1)
    packed = finish_sum(slab_slots, slab_copies)
    gram = unfold(packed[:RANK], packed[RANK : 2 * RANK], packed[2 * RANK : 2 * RANK + 1])

    share = remote(
        cross_full.at[parity], cross_full.at[parity], core_send.at[1], core_recv.at[1], sibling(0)
    )

    def share_cross():
        cross_full[parity] = finish_sum(cross_slots, cross_copies)
        share.start()

    ((mixing, own_gram),) = reduce_grams([gram], work, share_cross)
    mixes = at["mixes"]
    mixes[parity, :, : 2 * RANK] = mixing
    mixes[parity, :, 2 * RANK :] = own_gram
    swap = remote(mixes.at[parity], mixes.at[parity], core_send.at[2], core_recv.at[2], sibling(0))
    swap.start()
    share_far(0)
    prefix[...] = mix_rows(mixing, rows)
    share.wait()
    swap.wait()
    even, odd = mixes[0, :, : 2 * RANK], mixes[1, :, : 2 * RANK]
    crossed = jnp.concatenate([cross_full[0], cross_full[1]], 0)
    crossed = mm_t(mm(even, crossed), odd)
    ((mixing, new_gram),) = reduce_grams(
        [stack(mixes[0, :, 2 * RANK :], crossed, mixes[1, :, 2 * RANK :])],
        work,
        functools.partial(share_far, 1),
    )
    even, odd = mm(mixing[:, :RANK], even), mm(mixing[:, RANK:], odd)
    turns, far_turns = at["turns"], at["far_turns"]
    turns[:, : 2 * RANK] = even
    turns[:, 2 * RANK : 4 * RANK] = odd
    turns[:, 4 * RANK :] = new_gram
    turn_copies = [
        remote(
            source.at[part(1)], far_turns.at[part(1)], core_send.at[3 + hop], core_recv.at[3 + hop], sibling(hop)
        )
        for hop, source in ((1, turns), (0, far_turns))
    ]
    turn_copies[0].start()
    for piece in range(2, len(far_copies)):
        share_far(piece)
    block = mix_rows(jnp.where(parity == 0, even, odd), rows) + mix_rows(
        jnp.where(parity == 0, odd, even), other_rows
    )
    tree[1, :, :width] = block
    tree[1, :, width:] = new_gram
    prefix[...] = jnp.where(parity == 1, block, prefix[...])
    prefix_gram[...] = jnp.where(parity == 1, new_gram, own_gram)

    mine = part(under)
    size = RANK >> under
    count = min(4, size // 8)
    size = size // count
    near = [pl.ds(pl.multiple_of(mine.start + piece * size, size), size) for piece in range(count)]

    def lift(index, source, span, slot, other):
        return remote(
            source, lower.at[slot, span], up_send.at[index], up_recv.at[index], other
        )

    send_right = [
        lift(piece, tree.at[under, near[piece], pl.ds(0, width)], near[piece], 1, cousin)
        for piece in range(count)
    ]
    send_left = [
        lift(4 + piece, partner.at[under, near[piece], pl.ds(0, width)], near[piece], 0, cousin)
        for piece in range(count)
    ]
    pass_right = [
        lift(8 + piece, lower.at[1, near[piece]], near[piece], 1, sibling(under))
        for piece in range(count)
    ]
    pass_left = [
        lift(12 + piece, lower.at[0, near[piece]], near[piece], 0, sibling(under))
        for piece in range(count)
    ]
    sent, got = at["top_sent"], at["top_got"]
    above = [
        remote(sent.at[mine], got.at[mine], up_send.at[16 + index], up_recv.at[16], other)
        for index, other in enumerate((cousin, sibling(top)))
    ]
    shares = [
        [
            remote(
                ref.at[part(hop + 1)], ref.at[part(hop + 1)],
                share_send.at[slot, hop], share_recv.at[slot, hop], sibling(hop),
            )
            for slot, ref in enumerate((lower.at[0], lower.at[1], got))
        ]
        for hop in range(under - 1, -1, -1)
    ]

    def receive(level):
        if level > 1:
            fetch(level)
            return
        turn_copies[0].wait()
        turn_copies[1].start()
        for copy in far_shares:
            copy.wait()
        turn_copies[1].wait()
        partner[1, :, :width] = mix_rows(
            far_turns[:, : 2 * RANK], far_rows[0].astype(jnp.bfloat16)
        ) + mix_rows(far_turns[:, 2 * RANK : 4 * RANK], far_rows[1].astype(jnp.bfloat16))
        partner[1, :, width:] = far_turns[:, 4 * RANK :]

    for level in range(1, under):
        receive(level)
        other = partner[level, :, :width]
        other_gram = partner[level, :, width:]
        lefts = [(tree[level, :, :width], tree[level, :, width:]), (prefix[...], prefix_gram[...])]
        slots = at["twin_slots"].at[level - 1]
        for index, (left, _) in enumerate(lefts):
            slots[feat, index * RANK : (index + 1) * RANK, :] = overlap(left, other)
        crosses = finish_sum(slots, send_sum(slots, 1 + level))
        results = reduce_grams(
            [
                stack(left_gram, crosses[index * RANK : (index + 1) * RANK], other_gram)
                for index, (_, left_gram) in enumerate(lefts)
            ],
            work,
        )
        merged = [
            (blend(mixing, jnp.concatenate([left, other], 0)), new_gram)
            for (left, _), (mixing, new_gram) in zip(lefts, results)
        ]
        keep = bit_of(level) == 1
        prefix[...] = jnp.where(keep, merged[1][0], prefix[...])
        prefix_gram[...] = jnp.where(keep, merged[1][1], prefix_gram[...])
        tree[level + 1, :, :width] = merged[0][0]
        tree[level + 1, :, width:] = merged[0][1]

    @pl.when(is_lr)
    def _():
        for copy in send_right:
            copy.start()

    receive(under)

    @pl.when(is_lr)
    def _():
        for copy in send_left:
            copy.start()

    @pl.when(is_ul)
    def _():
        for copy, later in zip(send_right, pass_right):
            copy.wait_recv()
            later.start()
        shares[0][1].start()
        for copy, later in zip(send_left, pass_left):
            copy.wait_recv()
            later.start()
        shares[0][0].start()

    @pl.when(jnp.logical_not(is_ul))
    def _():
        other = partner[under, :, :width]
        full = bit_of(0)
        for bit in range(1, under):
            full = full * bit_of(bit)
        own = far & (full == 0)
        left = jnp.where(own, prefix[...], tree[under, :, :width])
        left_gram = jnp.where(own, prefix_gram[...], tree[under, :, width:])
        slots = at["level_slots"]
        slots[feat] = overlap(left, other)
        crossed = finish_sum(slots, send_sum(slots, top))

        def share_right():
            @pl.when(is_ur)
            def _():
                for copy in pass_right:
                    copy.wait_recv()
                shares[0][1].start()

        ((mixing, new_gram),) = reduce_grams(
            [stack(left_gram, crossed, partner[under, :, width:])], work, share_right
        )
        sent[:, : 2 * RANK] = mixing
        sent[:, 2 * RANK :] = new_gram

        @pl.when(is_ll)
        def _():
            for copy in above:
                copy.start()

        @pl.when(is_ur)
        def _():
            for copy in pass_left:
                copy.wait_recv()
            shares[0][0].start()

        @pl.when(far)
        def _():
            prefix[...] = blend(mixing, jnp.concatenate([left, other], 0))
            prefix_gram[...] = new_gram

    @pl.when(is_lr)
    def _():
        for copy in send_right + send_left:
            copy.wait_send()

    @pl.when(is_ll)
    def _():
        for copy in above:
            copy.wait_send()

    @pl.when(is_ul)
    def _():
        for copy in pass_right + pass_left:
            copy.wait_send()

    @pl.when(upper)
    def _():
        slots = at["top_slots"]
        copies = [None, None]
        for slot in (1, 0):
            for index, group in enumerate(shares):
                if index:
                    group[slot].start()
                group[slot].wait()
            slots[slot, feat] = overlap(lower[slot], prefix[...])
            copies[slot] = send_sum(slots.at[slot], 1 + top + 2 * slot)
        above[0].wait_recv()
        for index, group in enumerate(shares):
            group[2].start()
            if index == 0:
                crossed = jnp.concatenate(
                    [finish_sum(slots.at[slot], copies[slot]) for slot in range(2)], 0
                )
            group[2].wait()
        mixed = got[:, : 2 * RANK]
        crossed = mm(mixed, crossed)
        ((mixing, new_gram),) = reduce_grams(
            [stack(got[:, 2 * RANK :], crossed, prefix_gram[...])], work
        )
        mixed = mm(mixing[:, :RANK], mixed)
        prefix[...] = blend(
            jnp.concatenate([mixed, mixing[:, RANK:]], 1),
            jnp.concatenate([lower[0], lower[1], prefix[...]], 0),
        )
        prefix_gram[...] = new_gram

    ridge = ridge_ref[0, 0]
    seen_rows = ((seq + 1) * rows_ref.shape[0]).astype(jnp.float32)
    seen = jnp.full((1, 1), seen_rows * ridge, jnp.float32)
    half_basis = (prefix[...] * lax.rsqrt(seen)).astype(jnp.bfloat16)
    at["last_slots"][feat] = lax.dot_general(
        rows, half_basis, (((1,), (1,)), ((), ())), preferred_element_type=jnp.float32
    )
    copies = send_sum(at["last_slots"], 1 + levels)
    shifted = eye() + prefix_gram[...] / seen
    norm = jnp.sqrt(
        jnp.sum(jnp.sum(shifted * shifted, axis=1, keepdims=True), axis=0, keepdims=True)
    )

    work[0, :, :RANK] = shifted / norm
    work[0, :, RANK:] = eye()

    def root_step(index, carry):
        current, other = work[0, :, :RANK], work[0, :, RANK:]
        middle = 1.5 * eye() - 0.5 * mm_square(other, current)
        work[0, :, :RANK] = mm_square(current, middle)
        work[0, :, RANK:] = mm_square(middle, other)
        return carry

    lax.fori_loop(0, ROOT_STEPS, root_step, 0)
    current = work[0, :, :RANK]
    total_gram = shifted + current * jnp.sqrt(norm)
    total_gram = 0.5 * (total_gram + total_gram.T)
    (inverse,) = factorize([total_gram], work)
    projection = finish_sum(at["last_slots"], copies)
    coefficients = mm(mm_t(projection, inverse), inverse).astype(jnp.bfloat16)
    restored = jnp.dot(coefficients, half_basis, preferred_element_type=jnp.float32)
    out_ref[...] = (
        (rows.astype(jnp.float32) - restored) * lax.rsqrt(jnp.full((1, 1), ridge, jnp.float32))
    ).astype(jnp.bfloat16)


def on_device(activations, ridge_scale):
    tokens, width = activations.shape
    feats = lax.axis_size("feat")
    levels = lax.axis_size("seq").bit_length() - 1
    f32 = jnp.float32
    dma = pltpu.SemaphoreType.DMA
    scratch = dict(
        work=pltpu.VMEM((2, RANK, 2 * RANK), f32),
        tree=pltpu.VMEM((levels - 1, RANK, width + RANK), f32),
        partner=pltpu.VMEM((levels - 1, RANK, width + RANK), f32),
        prefix=pltpu.VMEM((RANK, width), f32),
        prefix_gram=pltpu.VMEM((RANK, RANK), f32),
        lower=pltpu.VMEM((2, RANK, width), f32),
        own_rows=pltpu.VMEM((tokens, width), f32),
        other_rows=pltpu.VMEM((tokens, width), f32),
        slab_slots=pltpu.VMEM((feats, 2 * RANK + 8, RANK), f32),
        far_rows=pltpu.VMEM((2, tokens, width), f32),
        turns=pltpu.VMEM((RANK, 5 * RANK), f32),
        far_turns=pltpu.VMEM((RANK, 5 * RANK), f32),
        cross_slots=pltpu.VMEM((feats, RANK, 2 * RANK), f32),
        cross_full=pltpu.VMEM((2, RANK, 2 * RANK), f32),
        mixes=pltpu.VMEM((2, RANK, 3 * RANK), f32),
        level_slots=pltpu.VMEM((feats, RANK, RANK), f32),
        top_sent=pltpu.VMEM((RANK, 3 * RANK), f32),
        top_got=pltpu.VMEM((RANK, 3 * RANK), f32),
        top_slots=pltpu.VMEM((2, feats, RANK, RANK), f32),
        last_slots=pltpu.VMEM((feats, tokens, RANK), f32),
        send_sem=dma((levels + 3, feats)),
        recv_sem=dma((levels + 3, feats)),
        pair_send=dma((levels, levels)),
        pair_recv=dma((levels, levels)),
        far_send=dma((2, 4)),
        far_recv=dma((2, 4)),
        core_send=dma((5,)),
        core_recv=dma((5,)),
        up_send=dma((18,)),
        up_recv=dma((18,)),
        share_send=dma((3, levels)),
        share_recv=dma((3, levels)),
    )
    if levels > 3:
        scratch["twin_slots"] = pltpu.VMEM((levels - 3, feats, 2 * RANK, RANK), f32)
    return pl.pallas_call(
        functools.partial(kernel, levels, feats, tuple(scratch)),
        out_shape=jax.ShapeDtypeStruct(activations.shape, activations.dtype),
        in_specs=[
            pl.BlockSpec(memory_space=pltpu.SMEM),
            pl.BlockSpec(memory_space=pltpu.VMEM),
        ],
        out_specs=pl.BlockSpec(memory_space=pltpu.VMEM),
        scratch_shapes=list(scratch.values()),
        compiler_params=pltpu.CompilerParams(
            collective_id=0, has_side_effects=True, vmem_limit_bytes=60 * 1024 * 1024
        ),
    )(ridge_scale.reshape(1, 1), activations)


def solution(mesh):
    placed = (P("seq", "feat"), P())
    return jax.shard_map(
        on_device, mesh=mesh, in_specs=placed, out_specs=P("seq", "feat"), check_vma=False
    )
```

```python
import functools

import jax
import jax.numpy as jnp
from jax import lax
from jax.experimental import pallas as pl
from jax.experimental.pallas import tpu as pltpu
from jax.sharding import PartitionSpec as P

RANK = 128
ROOT_STEPS = 12
BLOCK = 32
SUB = 16
MESH = pl.DeviceIdType.MESH
HIGHEST = lax.Precision.HIGHEST


def mm(a, b):
    return jnp.dot(a, b, precision=HIGHEST, preferred_element_type=jnp.float32)


def mm_t(a, b):
    return lax.dot_general(
        a, b, (((1,), (1,)), ((), ())), precision=HIGHEST, preferred_element_type=jnp.float32
    )


def mm_square(a, b):
    a_high, a_middle, a_low = split_3(a)
    b_high, b_middle, b_low = split_3(b)
    pair = jnp.concatenate([b_high, b_middle], 1)
    both = jnp.dot(
        jnp.concatenate([a_high, a_middle], 1),
        jnp.concatenate([pair, pair], 0),
        preferred_element_type=jnp.float32,
    )
    rest = jnp.dot(
        jnp.concatenate([a_high, a_low], 1),
        jnp.concatenate([b_low, b_high], 0),
        preferred_element_type=jnp.float32,
    )
    return both[:, :RANK] + (both[:, RANK:] + rest)


def split_3(x):
    high = x.astype(jnp.bfloat16)
    rest = x - high.astype(jnp.float32)
    middle = rest.astype(jnp.bfloat16)
    low = (rest - middle.astype(jnp.float32)).astype(jnp.bfloat16)
    return high, middle, low


def eye():
    rows = lax.broadcasted_iota(jnp.int32, (RANK, RANK), 0)
    columns = lax.broadcasted_iota(jnp.int32, (RANK, RANK), 1)
    return jnp.where(rows == columns, 1.0, 0.0).astype(jnp.float32)


def trace(matrix):
    size = matrix.shape[0]
    rows = lax.broadcasted_iota(jnp.int32, (size, size), 0)
    columns = lax.broadcasted_iota(jnp.int32, (size, size), 1)
    kept = jnp.where(rows == columns, matrix, 0.0)
    return jnp.sum(jnp.sum(kept, axis=1, keepdims=True), axis=0, keepdims=True)


def factorize(matrices, work, inverse=True):
    count = len(matrices)
    for k in range(count):
        work[k, :, :RANK] = matrices[k]
    lane = lax.broadcasted_iota(jnp.int32, (8, RANK), 1)
    sub = lax.broadcasted_iota(jnp.int32, (8, RANK), 0)
    rows = lax.broadcasted_iota(jnp.int32, (RANK, RANK), 0)
    cols_i = lax.broadcasted_iota(jnp.int32, (RANK, RANK), 1)
    groups = BLOCK // 8

    def step(index, carry):
        first = pl.multiple_of(index * BLOCK, BLOCK)
        here = lane - first
        left = [[work[k, pl.ds(first + 8 * g, 8), :RANK] for g in range(groups)] for k in range(count)]
        for start in range(0, BLOCK, SUB):
            active = range(start // 8, groups)
            columns = [
                [
                    {
                        g: jnp.broadcast_to(
                            jnp.sum(jnp.where(here == start + c, left[k][g], 0.0), axis=1, keepdims=True),
                            (8, RANK),
                        )
                        for g in active
                        if 8 * g + 7 >= start + c
                    }
                    for c in range(SUB)
                ]
                for k in range(count)
            ]
            if inverse:
                inside = (here >= start) & (here < start + SUB)
                for k in range(count):
                    for g in active:
                        unit = jnp.where(here == sub + 8 * g, 1.0, 0.0)
                        left[k][g] = jnp.where(inside, unit, left[k][g])
            for i in range(0, SUB, 2):
                at, row = divmod(start + i, 8)
                for k in range(count):
                    one, two = columns[k][i], columns[k][i + 1]
                    a = one[at][row : row + 1]
                    b = one[at][row + 1 : row + 2]
                    c = two[at][row + 1 : row + 2]
                    det = a * c - b * b
                    scale = lax.rsqrt(det)
                    inv = scale * scale
                    root = lax.rsqrt(a)
                    up, down = left[k][at][row : row + 1], left[k][at][row + 1 : row + 2]
                    for g in active:
                        if g < at or (g == at and row == 6):
                            continue
                        u = (c * one[g] - b * two[g]) * inv
                        v = (a * two[g] - b * one[g]) * inv
                        for j in range(i + 2, SUB):
                            if 8 * g + 7 >= start + j:
                                to, spot = divmod(start + j, 8)
                                columns[k][j][g] = columns[k][j][g] - (
                                    u * one[to][spot : spot + 1] + v * two[to][spot : spot + 1]
                                )
                        if g == at:
                            u = jnp.where(sub > row + 1, u, 0.0)
                            v = jnp.where(sub > row + 1, v, 0.0)
                        left[k][g] = left[k][g] - (u * up + v * down)
                    down = (a * down - b * up) * (root * scale)
                    left[k][at] = jnp.where(
                        sub == row, up * root, jnp.where(sub == row + 1, down, left[k][at])
                    )
        for k in range(count):
            if inverse:
                for g in range(SUB // 8):
                    left[k][g] = jnp.where((here >= SUB) & (here < BLOCK), 0.0, left[k][g])
            for g in range(groups):
                work[k, pl.ds(first + 8 * g, 8), :RANK] = left[k][g]

        @pl.when(index < RANK // BLOCK - 1)
        def _():
            for k in range(count):
                whole = jnp.concatenate(left[k], axis=0)
                wide = lax.broadcasted_iota(jnp.int32, (BLOCK, RANK), 1)
                a, b, c = split_3(whole)
                h, m, l = (jnp.where(wide >= first + BLOCK, part.astype(jnp.float32), 0.0) for part in (a, b, c))
                lhs = jnp.concatenate([h, h, m, m, h, l, jnp.zeros((2 * BLOCK, RANK), jnp.float32)], axis=0)
                lhs = lhs.astype(jnp.bfloat16).T
                rhs = jnp.concatenate([a, b, a, b, c, a, jnp.zeros((2 * BLOCK, RANK), jnp.bfloat16)], axis=0)
                update = jnp.dot(lhs, rhs, preferred_element_type=jnp.float32)
                old = work[k, :, :RANK]
                if inverse:
                    inside = (cols_i >= first) & (cols_i < first + BLOCK) & (rows >= first + BLOCK)
                    old = jnp.where(inside, 0.0, old)
                work[k, :, :RANK] = old - update
        return carry

    lax.fori_loop(0, RANK // BLOCK, step, 0)
    if inverse:
        return [jnp.where(cols_i <= rows, work[k, :, :RANK], 0.0) for k in range(count)]
    return [jnp.where(cols_i >= rows, work[k, :, :RANK], 0.0) for k in range(count)]


def reduce_grams(grams, work, between=None):
    scaled = [gram * (1.0 / trace(gram)) for gram in grams]
    images = [(gram[:RANK, :] + gram[RANK:, :]) * 0.7071067811865476 for gram in scaled]
    inverses = factorize([mm_t(image, image) for image in images], work)
    if between is not None:
        between()
    bases = [mm(inverse, image) for inverse, image in zip(inverses, images)]
    quotients = [mm_t(mm(basis, gram), basis) for basis, gram in zip(bases, scaled)]
    tails = [(trace(gram) - trace(quotient)) / RANK for gram, quotient in zip(scaled, quotients)]
    uppers = factorize(quotients, work, False)
    turned = [mm(upper, basis) for upper, basis in zip(uppers, bases)]
    inverses = factorize([mm_t(u, u) + tail * eye() for u, tail in zip(uppers, tails)], work)
    out = []
    for inverse, turn, gram in zip(inverses, turned, grams):
        mixing = mm(inverse, turn)
        out.append((mixing, mm_t(mm(mixing, gram), mixing)))
    return out


def mix_rows(mixing, rows):
    h, m, l = split_3(mixing)
    return (
        jnp.dot(l, rows, preferred_element_type=jnp.float32)
        + jnp.dot(m, rows, preferred_element_type=jnp.float32)
        + jnp.dot(h, rows, preferred_element_type=jnp.float32)
    )


def split_2(x):
    high = x.astype(jnp.bfloat16)
    return high, (x - high.astype(jnp.float32)).astype(jnp.bfloat16)


def blend(mixing, block):
    a, b = split_2(mixing)
    c, d = split_2(block)
    return (
        jnp.dot(b, c, preferred_element_type=jnp.float32)
        + jnp.dot(a, d, preferred_element_type=jnp.float32)
        + jnp.dot(a, c, preferred_element_type=jnp.float32)
    )


def overlap(first, second):
    a, b = split_2(first)
    c, d = split_2(second)
    dims = (((1,), (1,)), ((), ()))
    return (
        lax.dot_general(b, c, dims, preferred_element_type=jnp.float32)
        + lax.dot_general(a, d, dims, preferred_element_type=jnp.float32)
        + lax.dot_general(a, c, dims, preferred_element_type=jnp.float32)
    )


def stack(first, cross, last):
    return jnp.concatenate(
        [jnp.concatenate([first, cross], 1), jnp.concatenate([cross.T, last], 1)], 0
    )


def fold(gram):
    rows = lax.broadcasted_iota(jnp.int32, (RANK, RANK), 0)
    columns = lax.broadcasted_iota(jnp.int32, (RANK, RANK), 1)
    first, last = gram[:RANK, :RANK], gram[RANK:, RANK:]
    both = jnp.where(columns <= rows, first, last)
    diagonal = jnp.sum(jnp.where(columns == rows, last, 0.0), axis=0, keepdims=True)
    return both, gram[:RANK, RANK:], jnp.broadcast_to(diagonal, (8, RANK))


def unfold(both, cross, diagonal):
    rows = lax.broadcasted_iota(jnp.int32, (RANK, RANK), 0)
    columns = lax.broadcasted_iota(jnp.int32, (RANK, RANK), 1)
    turned = both.T
    first = jnp.where(columns <= rows, both, turned)
    last = jnp.where(columns > rows, both, jnp.where(columns < rows, turned, diagonal))
    return stack(first, cross, last)


def kernel(levels, feats, names, ridge_ref, rows_ref, out_ref, *scratch):
    at = dict(zip(names, scratch))
    work, tree, partner, prefix = at["work"], at["tree"], at["partner"], at["prefix"]
    prefix_gram, lower = at["prefix_gram"], at["lower"]
    send_sem, recv_sem = at["send_sem"], at["recv_sem"]
    pair_send, pair_recv = at["pair_send"], at["pair_recv"]
    core_send, core_recv = at["core_send"], at["core_recv"]
    up_send, up_recv = at["up_send"], at["up_recv"]
    share_send, share_recv = at["share_send"], at["share_recv"]
    seq = lax.axis_index("seq")
    feat = lax.axis_index("feat")
    width = rows_ref.shape[1]
    top, under = levels - 1, levels - 2

    def bit_of(level):
        return lax.rem(seq // (1 << level), 2)

    def flipped(level):
        return (1 << level) - 2 * (1 << level) * bit_of(level)

    def mirror(offset):
        if feats & (feats - 1):
            return lax.rem(feat + offset, feats)
        other = feat
        for bit in range(feats.bit_length() - 1):
            if offset >> bit & 1:
                other = other + (1 << bit) - 2 * (1 << bit) * lax.rem(feat // (1 << bit), 2)
        return other

    def sibling(level):
        return seq + flipped(level)

    cousin = seq + flipped(top) + flipped(under)
    upper = bit_of(top) == 1
    far = bit_of(under) == 1
    is_ll = (bit_of(top) == 0) & (bit_of(under) == 0)
    is_lr = (bit_of(top) == 0) & (bit_of(under) == 1)
    is_ul = (bit_of(top) == 1) & (bit_of(under) == 0)
    is_ur = (bit_of(top) == 1) & (bit_of(under) == 1)

    barrier = pltpu.get_barrier_semaphore()
    for offset in range(1, feats):
        pl.semaphore_signal(
            barrier, inc=1, device_id=(seq, lax.rem(feat + offset, feats)), device_id_type=MESH
        )
    for other in [sibling(level) for level in range(levels)] + [cousin]:
        pl.semaphore_signal(barrier, inc=1, device_id=(other, feat), device_id_type=MESH)
    rows = rows_ref[...]
    at["own_rows"][...] = rows.astype(jnp.float32)
    local = lax.dot_general(
        rows, rows, (((1,), (1,)), ((), ())), preferred_element_type=jnp.float32
    )
    pl.semaphore_wait(barrier, feats + levels)

    def remote(src, dst, sends, recvs, other):
        return pltpu.make_async_remote_copy(
            src_ref=src, dst_ref=dst, send_sem=sends, recv_sem=recvs,
            device_id=(other, feat), device_id_type=MESH,
        )

    def send_sum(slots, phase):
        copies = []
        for offset in range(feats - 1, 0, -1):
            copy = pltpu.make_async_remote_copy(
                src_ref=slots.at[feat],
                dst_ref=slots.at[feat],
                send_sem=send_sem.at[phase, offset],
                recv_sem=recv_sem.at[phase, offset],
                device_id=(seq, mirror(offset)),
                device_id_type=MESH,
            )
            copy.start()
            copies.append(copy)
        return copies

    def finish_sum(slots, copies):
        for copy in copies:
            copy.wait()
        total = slots[0]
        for index in range(1, feats):
            total = total + slots[index]
        return total

    def part(bits):
        size = RANK >> bits
        first = 0
        for bit in range(bits):
            first = first + bit_of(bit) * (RANK >> (bit + 1))
        return pl.ds(pl.multiple_of(first, size), size) if bits else pl.ds(0, RANK)

    def fetch(level):
        for index, hop in enumerate(range(level, -1, -1)):
            source = tree if hop == level else partner
            span = part(hop if hop == level else hop + 1)
            copy = remote(
                source.at[level, span], partner.at[level, span],
                pair_send.at[level, index], pair_recv.at[level, index], sibling(hop),
            )
            copy.start()
            copy.wait()

    parity = bit_of(0)
    rows_copy = remote(
        at["own_rows"], at["other_rows"], core_send.at[0], core_recv.at[0], sibling(0)
    )
    rows_copy.start()
    far_rows = at["far_rows"]
    pieces = far_rows.shape[1] // at["far_send"].shape[1]
    far_copies, far_shares = [], []
    for piece in range(at["far_send"].shape[1]):
        span = pl.ds(piece * pieces, pieces)
        far_copies.append(
            remote(
                at["own_rows"].at[span], far_rows.at[parity, span],
                at["far_send"].at[0, piece], at["far_recv"].at[0, piece], sibling(1),
            )
        )
        far_shares.append(
            remote(
                far_rows.at[parity, span], far_rows.at[parity, span],
                at["far_send"].at[1, piece], at["far_recv"].at[1, piece], sibling(0),
            )
        )
    for copy in far_copies:
        copy.start()

    def share_far(piece):
        far_copies[piece].wait()
        far_shares[piece].start()

    slab_slots, cross_slots, cross_full = at["slab_slots"], at["cross_slots"], at["cross_full"]
    both, between, diagonal = fold(local)
    slab_slots[feat, :RANK] = both
    slab_slots[feat, RANK : 2 * RANK] = between
    slab_slots[feat, 2 * RANK :] = diagonal
    slab_copies = send_sum(slab_slots, 0)
    rows_copy.wait()
    other_rows = at["other_rows"][...].astype(jnp.bfloat16)
    half = jnp.where(
        parity == 0, at["own_rows"][:RANK], at["other_rows"][RANK:]
    ).astype(jnp.bfloat16)
    odd_rows = jnp.where(parity == 0, at["other_rows"][...], at["own_rows"][...]).astype(jnp.bfloat16)
    cross_slots[feat] = lax.dot_general(
        half, odd_rows, (((1,), (1,)), ((), ())), preferred_element_type=jnp.float32
    )
    cross_copies = send_sum(cross_slots, 1)
    packed = finish_sum(slab_slots, slab_copies)
    gram = unfold(packed[:RANK], packed[RANK : 2 * RANK], packed[2 * RANK : 2 * RANK + 1])

    share = remote(
        cross_full.at[parity], cross_full.at[parity], core_send.at[1], core_recv.at[1], sibling(0)
    )

    def share_cross():
        cross_full[parity] = finish_sum(cross_slots, cross_copies)
        share.start()

    ((mixing, own_gram),) = reduce_grams([gram], work, share_cross)
    mixes = at["mixes"]
    mixes[parity, :, : 2 * RANK] = mixing
    mixes[parity, :, 2 * RANK :] = own_gram
    swap = remote(mixes.at[parity], mixes.at[parity], core_send.at[2], core_recv.at[2], sibling(0))
    swap.start()
    share_far(0)
    prefix[...] = mix_rows(mixing, rows)
    share.wait()
    swap.wait()
    even, odd = mixes[0, :, : 2 * RANK], mixes[1, :, : 2 * RANK]
    crossed = jnp.concatenate([cross_full[0], cross_full[1]], 0)
    crossed = mm_t(mm(even, crossed), odd)
    ((mixing, new_gram),) = reduce_grams(
        [stack(mixes[0, :, 2 * RANK :], crossed, mixes[1, :, 2 * RANK :])],
        work,
        functools.partial(share_far, 1),
    )
    even, odd = mm(mixing[:, :RANK], even), mm(mixing[:, RANK:], odd)
    turns, far_turns = at["turns"], at["far_turns"]
    turns[:, : 2 * RANK] = even
    turns[:, 2 * RANK : 4 * RANK] = odd
    turns[:, 4 * RANK :] = new_gram
    turn_copies = [
        remote(
            source.at[part(1)], far_turns.at[part(1)], core_send.at[3 + hop], core_recv.at[3 + hop], sibling(hop)
        )
        for hop, source in ((1, turns), (0, far_turns))
    ]
    turn_copies[0].start()
    for piece in range(2, len(far_copies)):
        share_far(piece)
    block = mix_rows(jnp.where(parity == 0, even, odd), rows) + mix_rows(
        jnp.where(parity == 0, odd, even), other_rows
    )
    tree[1, :, :width] = block
    tree[1, :, width:] = new_gram
    prefix[...] = jnp.where(parity == 1, block, prefix[...])
    prefix_gram[...] = jnp.where(parity == 1, new_gram, own_gram)

    mine = part(under)
    size = RANK >> under
    count = min(4, size // 8)
    size = size // count
    near = [pl.ds(pl.multiple_of(mine.start + piece * size, size), size) for piece in range(count)]

    def lift(index, source, span, slot, other):
        return remote(
            source, lower.at[slot, span], up_send.at[index], up_recv.at[index], other
        )

    send_right = [
        lift(piece, tree.at[under, near[piece], pl.ds(0, width)], near[piece], 1, cousin)
        for piece in range(count)
    ]
    send_left = [
        lift(4 + piece, partner.at[under, near[piece], pl.ds(0, width)], near[piece], 0, cousin)
        for piece in range(count)
    ]
    pass_right = [
        lift(8 + piece, lower.at[1, near[piece]], near[piece], 1, sibling(under))
        for piece in range(count)
    ]
    pass_left = [
        lift(12 + piece, lower.at[0, near[piece]], near[piece], 0, sibling(under))
        for piece in range(count)
    ]
    sent, got = at["top_sent"], at["top_got"]
    above = [
        remote(sent.at[mine], got.at[mine], up_send.at[16 + index], up_recv.at[16], other)
        for index, other in enumerate((cousin, sibling(top)))
    ]
    shares = [
        [
            remote(
                ref.at[part(hop + 1)], ref.at[part(hop + 1)],
                share_send.at[slot, hop], share_recv.at[slot, hop], sibling(hop),
            )
            for slot, ref in enumerate((lower.at[0], lower.at[1], got))
        ]
        for hop in range(under - 1, -1, -1)
    ]

    def receive(level):
        if level > 1:
            fetch(level)
            return
        turn_copies[0].wait()
        turn_copies[1].start()
        for copy in far_shares:
            copy.wait()
        turn_copies[1].wait()
        partner[1, :, :width] = mix_rows(
            far_turns[:, : 2 * RANK], far_rows[0].astype(jnp.bfloat16)
        ) + mix_rows(far_turns[:, 2 * RANK : 4 * RANK], far_rows[1].astype(jnp.bfloat16))
        partner[1, :, width:] = far_turns[:, 4 * RANK :]

    for level in range(1, under):
        receive(level)
        other = partner[level, :, :width]
        other_gram = partner[level, :, width:]
        lefts = [(tree[level, :, :width], tree[level, :, width:]), (prefix[...], prefix_gram[...])]
        slots = at["twin_slots"].at[level - 1]
        for index, (left, _) in enumerate(lefts):
            slots[feat, index * RANK : (index + 1) * RANK, :] = overlap(left, other)
        crosses = finish_sum(slots, send_sum(slots, 1 + level))
        results = reduce_grams(
            [
                stack(left_gram, crosses[index * RANK : (index + 1) * RANK], other_gram)
                for index, (_, left_gram) in enumerate(lefts)
            ],
            work,
        )
        merged = [
            (blend(mixing, jnp.concatenate([left, other], 0)), new_gram)
            for (left, _), (mixing, new_gram) in zip(lefts, results)
        ]
        keep = bit_of(level) == 1
        prefix[...] = jnp.where(keep, merged[1][0], prefix[...])
        prefix_gram[...] = jnp.where(keep, merged[1][1], prefix_gram[...])
        tree[level + 1, :, :width] = merged[0][0]
        tree[level + 1, :, width:] = merged[0][1]

    @pl.when(is_lr)
    def _():
        for copy in send_right:
            copy.start()

    receive(under)

    @pl.when(is_lr)
    def _():
        for copy in send_left:
            copy.start()

    @pl.when(is_ul)
    def _():
        for copy, later in zip(send_right, pass_right):
            copy.wait_recv()
            later.start()
        shares[0][1].start()
        for copy, later in zip(send_left, pass_left):
            copy.wait_recv()
            later.start()
        shares[0][0].start()

    @pl.when(jnp.logical_not(is_ul))
    def _():
        other = partner[under, :, :width]
        full = bit_of(0)
        for bit in range(1, under):
            full = full * bit_of(bit)
        own = far & (full == 0)
        left = jnp.where(own, prefix[...], tree[under, :, :width])
        left_gram = jnp.where(own, prefix_gram[...], tree[under, :, width:])
        slots = at["level_slots"]
        slots[feat] = overlap(left, other)
        crossed = finish_sum(slots, send_sum(slots, top))

        def share_right():
            @pl.when(is_ur)
            def _():
                for copy in pass_right:
                    copy.wait_recv()
                shares[0][1].start()

        ((mixing, new_gram),) = reduce_grams(
            [stack(left_gram, crossed, partner[under, :, width:])], work, share_right
        )
        sent[:, : 2 * RANK] = mixing
        sent[:, 2 * RANK :] = new_gram

        @pl.when(is_ll)
        def _():
            for copy in above:
                copy.start()

        @pl.when(is_ur)
        def _():
            for copy in pass_left:
                copy.wait_recv()
            shares[0][0].start()

        @pl.when(far)
        def _():
            prefix[...] = blend(mixing, jnp.concatenate([left, other], 0))
            prefix_gram[...] = new_gram

    @pl.when(is_lr)
    def _():
        for copy in send_right + send_left:
            copy.wait_send()

    @pl.when(is_ll)
    def _():
        for copy in above:
            copy.wait_send()

    @pl.when(is_ul)
    def _():
        for copy in pass_right + pass_left:
            copy.wait_send()

    @pl.when(upper)
    def _():
        slots = at["top_slots"]
        copies = [None, None]
        for slot in (1, 0):
            for index, group in enumerate(shares):
                if index:
                    group[slot].start()
                group[slot].wait()
            slots[slot, feat] = overlap(lower[slot], prefix[...])
            copies[slot] = send_sum(slots.at[slot], 1 + top + 2 * slot)
        above[0].wait_recv()
        for index, group in enumerate(shares):
            group[2].start()
            if index == 0:
                crossed = jnp.concatenate(
                    [finish_sum(slots.at[slot], copies[slot]) for slot in range(2)], 0
                )
            group[2].wait()
        mixed = got[:, : 2 * RANK]
        crossed = mm(mixed, crossed)
        ((mixing, new_gram),) = reduce_grams(
            [stack(got[:, 2 * RANK :], crossed, prefix_gram[...])], work
        )
        mixed = mm(mixing[:, :RANK], mixed)
        prefix[...] = blend(
            jnp.concatenate([mixed, mixing[:, RANK:]], 1),
            jnp.concatenate([lower[0], lower[1], prefix[...]], 0),
        )
        prefix_gram[...] = new_gram

    ridge = ridge_ref[0, 0]
    seen_rows = ((seq + 1) * rows_ref.shape[0]).astype(jnp.float32)
    seen = jnp.full((1, 1), seen_rows * ridge, jnp.float32)
    half_basis = (prefix[...] * lax.rsqrt(seen)).astype(jnp.bfloat16)
    at["last_slots"][feat] = lax.dot_general(
        rows, half_basis, (((1,), (1,)), ((), ())), preferred_element_type=jnp.float32
    )
    copies = send_sum(at["last_slots"], 1 + levels)
    shifted = eye() + prefix_gram[...] / seen
    norm = jnp.sqrt(
        jnp.sum(jnp.sum(shifted * shifted, axis=1, keepdims=True), axis=0, keepdims=True)
    )

    work[0, :, :RANK] = shifted / norm
    work[0, :, RANK:] = eye()

    def root_step(index, carry):
        current, other = work[0, :, :RANK], work[0, :, RANK:]
        middle = 1.5 * eye() - 0.5 * mm_square(other, current)
        work[0, :, :RANK] = mm_square(current, middle)
        work[0, :, RANK:] = mm_square(middle, other)
        return carry

    lax.fori_loop(0, ROOT_STEPS, root_step, 0)
    current = work[0, :, :RANK]
    total_gram = shifted + current * jnp.sqrt(norm)
    total_gram = 0.5 * (total_gram + total_gram.T)
    (inverse,) = factorize([total_gram], work)
    projection = finish_sum(at["last_slots"], copies)
    coefficients = mm(mm_t(projection, inverse), inverse).astype(jnp.bfloat16)
    restored = jnp.dot(coefficients, half_basis, preferred_element_type=jnp.float32)
    out_ref[...] = (
        (rows.astype(jnp.float32) - restored) * lax.rsqrt(jnp.full((1, 1), ridge, jnp.float32))
    ).astype(jnp.bfloat16)


def on_device(activations, ridge_scale):
    tokens, width = activations.shape
    feats = lax.axis_size("feat")
    levels = lax.axis_size("seq").bit_length() - 1
    f32 = jnp.float32
    dma = pltpu.SemaphoreType.DMA
    scratch = dict(
        work=pltpu.VMEM((2, RANK, 2 * RANK), f32),
        tree=pltpu.VMEM((levels - 1, RANK, width + RANK), f32),
        partner=pltpu.VMEM((levels - 1, RANK, width + RANK), f32),
        prefix=pltpu.VMEM((RANK, width), f32),
        prefix_gram=pltpu.VMEM((RANK, RANK), f32),
        lower=pltpu.VMEM((2, RANK, width), f32),
        own_rows=pltpu.VMEM((tokens, width), f32),
        other_rows=pltpu.VMEM((tokens, width), f32),
        slab_slots=pltpu.VMEM((feats, 2 * RANK + 8, RANK), f32),
        far_rows=pltpu.VMEM((2, tokens, width), f32),
        turns=pltpu.VMEM((RANK, 5 * RANK), f32),
        far_turns=pltpu.VMEM((RANK, 5 * RANK), f32),
        cross_slots=pltpu.VMEM((feats, RANK, 2 * RANK), f32),
        cross_full=pltpu.VMEM((2, RANK, 2 * RANK), f32),
        mixes=pltpu.VMEM((2, RANK, 3 * RANK), f32),
        level_slots=pltpu.VMEM((feats, RANK, RANK), f32),
        top_sent=pltpu.VMEM((RANK, 3 * RANK), f32),
        top_got=pltpu.VMEM((RANK, 3 * RANK), f32),
        top_slots=pltpu.VMEM((2, feats, RANK, RANK), f32),
        last_slots=pltpu.VMEM((feats, tokens, RANK), f32),
        send_sem=dma((levels + 3, feats)),
        recv_sem=dma((levels + 3, feats)),
        pair_send=dma((levels, levels)),
        pair_recv=dma((levels, levels)),
        far_send=dma((2, 4)),
        far_recv=dma((2, 4)),
        core_send=dma((5,)),
        core_recv=dma((5,)),
        up_send=dma((18,)),
        up_recv=dma((18,)),
        share_send=dma((3, levels)),
        share_recv=dma((3, levels)),
    )
    if levels > 3:
        scratch["twin_slots"] = pltpu.VMEM((levels - 3, feats, 2 * RANK, RANK), f32)
    return pl.pallas_call(
        functools.partial(kernel, levels, feats, tuple(scratch)),
        out_shape=jax.ShapeDtypeStruct(activations.shape, activations.dtype),
        in_specs=[
            pl.BlockSpec(memory_space=pltpu.SMEM),
            pl.BlockSpec(memory_space=pltpu.VMEM),
        ],
        out_specs=pl.BlockSpec(memory_space=pltpu.VMEM),
        scratch_shapes=list(scratch.values()),
        compiler_params=pltpu.CompilerParams(
            collective_id=0, has_side_effects=True, vmem_limit_bytes=60 * 1024 * 1024
        ),
    )(ridge_scale.reshape(1, 1), activations)


def solution(mesh):
    placed = (P("seq", "feat"), P())
    return jax.shard_map(
        on_device, mesh=mesh, in_specs=placed, out_specs=P("seq", "feat"), check_vma=False
    )
```
